128 devices in a mesh: row: 8 (over x, core), col: 16 (over z, y).
Axes of the slice: x: 4, y: 4, z: 4, core: 2. Of those that a mesh axis runs over, the one named last changes fastest.
Arguments:
- rhs: float32 [32, 1048576], P(None, ('row', 'col')), may hold values from -12.5 to 12.5
- near_blocks: bfloat16 [16384, 4, 4096], P(('row', 'col')), may hold values from -0.1875 to 0.1875
- near_offsets: int32 [16384, 4], P(('row', 'col')), may hold values from -4 to 4, as said below
- v_factor: bfloat16 [16384, 2048], P(('row', 'col')), may hold values from -0.75 to 0.75
- mix_col: bfloat16 [8, 128, 512, 512], P('row', 'col'), may hold values from -0.25 to 0.25
- mix_row: bfloat16 [8, 256, 256, 256], P('row', 'col'), may hold values from -0.375 to 0.375
- u_factor: bfloat16 [16384, 2048], P(('row', 'col')), may hold values from -0.75 to 0.75
Outputs:
- solution: float32 [32, 1048576], P(None, ('row', 'col'))
- residual: float32 [32, 1048576], P(None, ('row', 'col'))
The draws below stay inside these ranges and needn't reach their ends.
Inputs may be any that keep to these rules, and one draw needn't show every extreme that they name: `near_offsets`: column 0 is 0; the other entries of a row are distinct and nonzero. In every aligned block of 128 rows some row holds -4 and some row holds 4.
All inputs are finite; a program needn't handle non-finite values.
Results may differ from the reference program's by a relative error of at most 0.0054.
Values may be sent and summed in bfloat16 or wider, within the bound.
A program may use at most 128 MiB of HBM per device.

```python
import jax
import jax.numpy as jnp
from jax import lax

RHS = 32
LEAF = 64
RANK = 32
NNEAR = 4
HALO = 4
LEAVES_DEV = 128
NLEAVES = 16384
N_UNKNOWNS = 1048576
SLOTS = 8
SUBSLOTS = 1
N_ROW = 8
N_COL = 16
DEVICES = 128


def draw_rhs(key, part):
    scale_key = jax.random.fold_in(key, 11)
    value_key = jax.random.fold_in(key, 12)
    scales = jnp.exp(jax.random.uniform(scale_key, (DEVICES,), jnp.float32, jnp.log(0.2), jnp.log(2.5)))
    scales = jnp.repeat(scales, N_UNKNOWNS // DEVICES)[None, :]
    values = jnp.clip(jax.random.normal(value_key, (RHS, N_UNKNOWNS), jnp.float32), -5.0, 5.0)
    return (values * scales).astype(jnp.float32)


def draw_near_offsets(key, part):
    score_key = jax.random.fold_in(key, 21)
    choices_count = 2 * HALO
    column = jnp.arange(choices_count, dtype=jnp.int32)
    candidates = jnp.where(column < HALO, column - HALO, column - HALO + 1)
    scores = jax.random.randint(score_key, (NLEAVES, choices_count), 0, 2 ** 20, dtype=jnp.int32) * choices_count + column[None, :]
    leading = (jnp.arange(NLEAVES, dtype=jnp.int32) % LEAVES_DEV == 0)[:, None]
    forced = jnp.where(column == 0, -2, jnp.where(column == choices_count - 1, -1, scores))
    scores = jnp.where(leading, forced, scores)
    order = jnp.argsort(scores, axis=1)
    picked = candidates[order[:, :NNEAR - 1]]
    return jnp.concatenate([jnp.zeros((NLEAVES, 1), jnp.int32), picked.astype(jnp.int32)], axis=1)


def shard_levels(stream_key, dims, shards, low, largest):
    loudness = 1.0
    for axis_at, shards_of in shards:
        draws = jax.random.uniform(jax.random.fold_in(jax.random.fold_in(stream_key, 6), axis_at), (shards_of,), jnp.float32, low / len(shards), largest / len(shards))
        loudness = loudness * jnp.repeat(jnp.exp(draws), dims[axis_at] // shards_of).reshape((-1,) + (1,) * (len(dims) - 1 - axis_at))
    return loudness


def normal_values(rng, shape, scale, most, split=(), held_as=jnp.bfloat16):
    level = shard_levels(rng, shape, split, -0.22, 0.18) if split else 1.0
    values = jax.random.normal(rng, shape, jnp.float32) * scale * level
    return jnp.minimum(jnp.maximum(values, -most), most).astype(held_as)


def setup_inputs(seed: int = 0) -> dict:
    arg_keys = jax.random.split(jax.random.key(seed), 8)
    rhs = draw_rhs(jax.random.fold_in(arg_keys[7], 71), 0)
    near_blocks = normal_values(arg_keys[1], (NLEAVES, NNEAR, LEAF * LEAF), (4 * NNEAR * LEAF) ** -0.5, 0.1875, ((0, 128),))
    near_offsets = draw_near_offsets(jax.random.fold_in(arg_keys[7], 71), 0)
    v_factor = normal_values(arg_keys[3], (NLEAVES, LEAF * RANK), LEAF ** -0.5, 0.75, ((0, 128),))
    mix_col = normal_values(arg_keys[4], (N_ROW, N_COL * SLOTS, N_COL * RANK, N_COL * RANK), (N_COL * RANK) ** -0.5, 0.25, ((0, 8), (1, 16)))
    mix_row = normal_values(arg_keys[5], (N_ROW * SUBSLOTS, N_COL * N_COL, N_ROW * RANK, N_ROW * RANK), (N_ROW * RANK) ** -0.5, 0.375, ((0, 8), (1, 16)))
    u_factor = normal_values(arg_keys[6], (NLEAVES, RANK * LEAF), (2 * RANK) ** -0.5, 0.75, ((0, 128),))
    return {"rhs": rhs, "near_blocks": near_blocks, "near_offsets": near_offsets, "v_factor": v_factor, "mix_col": mix_col, "mix_row": mix_row, "u_factor": u_factor}


def near_term(vector_bf, near_blocks, near_offsets):
    padded = jnp.pad(vector_bf, ((0, 0), (HALO * LEAF, HALO * LEAF)))
    padded = padded.reshape(RHS, NLEAVES + 2 * HALO, LEAF)
    blocks = near_blocks.reshape(DEVICES, LEAVES_DEV, NNEAR, LEAF, LEAF)
    offsets = near_offsets.reshape(DEVICES, LEAVES_DEV, NNEAR)

    def one_block(device):
        position = device * LEAVES_DEV + jnp.arange(LEAVES_DEV, dtype=jnp.int32)[:, None] + offsets[device] + HALO
        picked = padded[:, position, :].astype(jnp.float32)
        return jnp.einsum('slnu,lnvu->slv', picked, blocks[device].astype(jnp.float32))
    result = lax.map(one_block, jnp.arange(DEVICES, dtype=jnp.int32))
    return jnp.transpose(result, (1, 0, 2, 3)).reshape(RHS, N_UNKNOWNS)

def far_term(vector_bf, v_factor, mix_col, mix_row, u_factor):
    width_col = N_COL * RANK
    width_row = N_ROW * RANK
    local = vector_bf.reshape(RHS, NLEAVES, LEAF).astype(jnp.float32)
    factor = v_factor.reshape(NLEAVES, LEAF, RANK).astype(jnp.float32)
    coeffs = jnp.einsum('slu,luk->lsk', local, factor).astype(jnp.bfloat16)
    coeffs = coeffs.reshape(N_ROW, N_COL, N_COL, SLOTS, RHS, RANK)
    first_mix = mix_col.reshape(N_ROW, N_COL, SLOTS, N_COL, RANK, width_col)

    def level_one(rowgrp):
        return jnp.einsum('cgjsk,gjckm->gjsm', coeffs[rowgrp].astype(jnp.float32), first_mix[rowgrp].astype(jnp.float32)).astype(jnp.bfloat16)
    first = lax.map(level_one, jnp.arange(N_ROW, dtype=jnp.int32))
    first = first.reshape(N_ROW, N_COL, N_ROW, SUBSLOTS, RHS, N_COL, RANK)
    second_mix = mix_row.reshape(N_ROW, SUBSLOTS, N_COL, N_COL, N_ROW, RANK, width_row)
    expand = u_factor.reshape(N_ROW, N_COL, SUBSLOTS, N_COL, N_ROW, RANK, LEAF)

    def level_two(target):
        picked = lax.dynamic_index_in_dim(first, target, 2, keepdims=False)
        second = jnp.einsum('rgjspk,jgprkn->gjpsn', picked.astype(jnp.float32), second_mix[target].astype(jnp.float32)).astype(jnp.bfloat16)
        second = second.reshape(N_COL, SUBSLOTS, N_COL, RHS, N_ROW, RANK)
        out = jnp.einsum('gjpsqk,gjpqku->sgjpqu', second.astype(jnp.float32), expand[target].astype(jnp.float32))
        return out.reshape(RHS, N_COL * LEAVES_DEV * LEAF)
    result = lax.map(level_two, jnp.arange(N_ROW, dtype=jnp.int32))
    return jnp.transpose(result, (1, 0, 2)).reshape(RHS, N_UNKNOWNS)

def reference(rhs, near_blocks, near_offsets, v_factor, mix_col, mix_row, u_factor):

    def operator(vector):
        vector_bf = vector.astype(jnp.bfloat16)
        return vector + near_term(vector_bf, near_blocks, near_offsets) + far_term(vector_bf, v_factor, mix_col, mix_row, u_factor)
    rhs_length = jnp.sqrt(lax.optimization_barrier(jnp.sum(rhs * rhs, axis=1)))
    basis_first = rhs / rhs_length[:, None]
    image_first = operator(basis_first)
    h_one_one = lax.optimization_barrier(jnp.sum(basis_first * image_first, axis=1))
    rest_first = image_first - h_one_one[:, None] * basis_first
    h_two_one = jnp.sqrt(lax.optimization_barrier(jnp.sum(rest_first * rest_first, axis=1)))
    basis_second = rest_first / h_two_one[:, None]
    image_second = operator(basis_second)
    h_one_two = lax.optimization_barrier(jnp.sum(basis_first * image_second, axis=1))
    h_two_two = lax.optimization_barrier(jnp.sum(basis_second * image_second, axis=1))
    rest_second = image_second - h_one_two[:, None] * basis_first - h_two_two[:, None] * basis_second
    h_three_two = jnp.sqrt(lax.optimization_barrier(jnp.sum(rest_second * rest_second, axis=1)))
    m_first = h_one_one * h_one_one + h_two_one * h_two_one
    m_cross = h_one_one * h_one_two + h_two_one * h_two_two
    m_second = h_one_two * h_one_two + h_two_two * h_two_two + h_three_two * h_three_two
    determ = m_first * m_second - m_cross * m_cross
    coef_first = rhs_length * (m_second * h_one_one - m_cross * h_one_two) / determ
    coef_second = rhs_length * (m_first * h_one_two - m_cross * h_one_one) / determ
    solution = coef_first[:, None] * basis_first + coef_second[:, None] * basis_second
    residual = rhs - coef_first[:, None] * image_first - coef_second[:, None] * image_second
    return (solution, residual)
```

```python
import functools

import jax
import jax.numpy as jnp
from jax import lax
from jax.experimental import pallas as pl
from jax.experimental.pallas import tpu as pltpu
from jax.sharding import PartitionSpec as P

S = 32
LEAF = 64
RANK = 32
HALO = 4
F32 = jnp.float32
BF16 = jnp.bfloat16
MESH = pl.DeviceIdType.MESH
NT = (((1,), (1,)), ((), ()))


def dot(a, b):
    return jnp.dot(a, b, preferred_element_type=F32)


def lane_index():
    return lax.broadcasted_iota(jnp.int32, (S, 128), 1)


def blocks_swapped(tiles):
    lane = lane_index()
    low_half = lane < 64
    low_quarter = lax.rem(lane, 64) < 32
    a, b, c, d = tiles
    turn = lambda x, by: pltpu.roll(x, by, 1)
    a, c = jnp.where(low_half, a, turn(c, 64)), jnp.where(low_half, turn(a, 64), c)
    b, d = jnp.where(low_half, b, turn(d, 64)), jnp.where(low_half, turn(b, 64), d)
    a, b = jnp.where(low_quarter, a, turn(b, 32)), jnp.where(low_quarter, turn(a, 96), b)
    c, d = jnp.where(low_quarter, c, turn(d, 32)), jnp.where(low_quarter, turn(c, 96), d)
    return a, b, c, d


def kernel(
    n_row, n_col,
    r_hbm, w_hbm, off, v_hbm, mc_hbm, mr_hbm, u_hbm,
    sol, res,
    rv, bv, dv, wraw, wp, vraw, vq, uraw, uq, mc, mr, xlo, xhi,
    hs, hr, zs, zr, zt, ts, tr, tt, sa, sb, g1, h1, g2, h2,
    load_sem, hs_sem, hr_sem, zs_sem, zr_sem, ts_sem, tr_sem, g_sem, h_sem,
):
    row = lax.axis_index("row")
    col = lax.axis_index("col")
    flat = row * n_col + col
    total = n_row * n_col
    leaves = off.shape[1]
    lane = lane_index()
    low_half = lane < 64

    def loads(index, src, dst):
        copy = pltpu.make_async_copy(src, dst, load_sem.at[index])
        copy.start()
        return copy

    v_load = loads(0, v_hbm, vraw)
    r_load = loads(1, r_hbm, rv)
    w_load = loads(2, w_hbm, wraw)
    mc_load = loads(3, mc_hbm, mc)
    mr_load = loads(4, mr_hbm, mr)
    u_load = loads(5, u_hbm, uraw)

    def other_col(k):
        return lax.rem(col + k, n_col)

    def other_row(k):
        return lax.rem(row + k, n_row)

    def at_flat(k):
        other = lax.rem(flat + k, total)
        return (lax.div(other, n_col), lax.rem(other, n_col))

    up, down = at_flat(1), at_flat(total - 1)
    barrier = pltpu.get_barrier_semaphore()
    partners = [(row, other_col(k)) for k in range(1, n_col)]
    partners += [(other_row(k), col) for k in range(1, n_row)] + [up, down]
    for partner in partners:
        pl.semaphore_signal(barrier, inc=1, device_id=partner, device_id_type=MESH)

    sends = []

    def send(src, dst, send_sem, recv_sem, device):
        copy = pltpu.make_async_remote_copy(
            src_ref=src, dst_ref=dst, send_sem=send_sem, recv_sem=recv_sem,
            device_id=device, device_id_type=MESH,
        )
        copy.start()
        sends.append(copy)

    def arrived(dst, send_sem, recv_sem):
        pltpu.make_async_remote_copy(
            src_ref=dst, dst_ref=dst, send_sem=send_sem, recv_sem=recv_sem,
            device_id=(row, col), device_id_type=MESH,
        ).wait_recv()

    def expand_v():
        group = lax.broadcasted_iota(jnp.int32, (16, 128), 1) // RANK

        def step(at, _):
            sa[0] = vraw[pl.ds(pl.multiple_of(at * 128, 128), 128), :].astype(F32)
            for leaf in range(8):
                j = leaf % 4
                part = sa[0, pl.ds(leaf, 16, stride=8), :]
                for w in range(4):
                    turned = part if j == w else pltpu.roll(part, ((j - w) % 4) * RANK, 1)
                    sb[2 * (leaf // 4) + j // 2, pl.ds((j % 2) * 64 + w, 16, stride=4), :] = jnp.where(
                        group == j, turned, 0.0
                    )
            for q in range(4):
                vq[pl.ds(pl.multiple_of(at * 512 + q * 128, 128), 128), :] = sb[q].astype(BF16)
            return 0

        lax.fori_loop(0, leaves // 8, step, 0)

    def expand_u():
        half = lax.broadcasted_iota(jnp.int32, (16, 128), 1) // LEAF
        nothing = jnp.zeros((64, 128), BF16)

        def step(at, _):
            sa[0] = uraw[pl.ds(pl.multiple_of(at * 128, 128), 128), :].astype(F32)
            for leaf in range(8):
                q = leaf % 4
                part = sa[0, pl.ds(leaf, 16, stride=8), :]
                turned = pltpu.roll(part, 64, 1)
                for w in range(2):
                    sb[leaf // 4, pl.ds(q * RANK + w, 16, stride=2), :] = jnp.where(
                        half == q % 2, part if w == q % 2 else turned, 0.0
                    )
            for q in range(2):
                base = pl.multiple_of(at * 256 + q * 128, 128)
                uq[pl.ds(base, 64), 0:128] = sb[q, 0:64].astype(BF16)
                uq[pl.ds(base, 64), 128:256] = nothing
                uq[pl.ds(base + 64, 64), 0:128] = nothing
                uq[pl.ds(base + 64, 64), 128:256] = sb[q, 64:128].astype(BF16)
            return 0

        lax.fori_loop(0, leaves // 8, step, 0)

    def expand_w(first, last):
        half = lax.broadcasted_iota(jnp.int32, (32, 128), 1) < 64

        def step(at, _):
            for k in range(4):
                leaf = at * 4 + k
                sa[k] = wraw[pl.ds(pl.multiple_of(leaf * 128, 128), 128), :].astype(F32)
            for k in range(4):
                leaf = at * 4 + k
                for b in range(2):
                    one = sa[k, pl.ds(2 * b, 32, stride=4), :]
                    two = sa[k, pl.ds(2 * b + 1, 32, stride=4), :]
                    sb[k, pl.ds(64 * b, 32, stride=2), :] = jnp.where(half, one, pltpu.roll(two, 64, 1))
                    sb[k, pl.ds(64 * b + 1, 32, stride=2), :] = jnp.where(half, pltpu.roll(one, 64, 1), two)
            for k in range(4):
                base = pl.multiple_of((at * 4 + k) * 64, 64)
                wp[pl.ds(base, 64), 0:128] = sb[k, 0:64].astype(BF16)
                wp[pl.ds(base, 64), 128:256] = sb[k, 64:128].astype(BF16)
            return 0

        lax.fori_loop(first, last, step, 0)

    def send_edges(app, src):
        hs[app, 0] = src[:, 0 : HALO * LEAF].astype(BF16)
        hs[app, 1] = src[:, (leaves - HALO) * LEAF : leaves * LEAF].astype(BF16)
        send(hs.at[app, 0], hr.at[app, 1], hs_sem.at[app, 0], hr_sem.at[app, 1], down)
        send(hs.at[app, 1], hr.at[app, 0], hs_sem.at[app, 1], hr_sem.at[app, 0], up)

    def compress(app, src, k_range):
        outs = []
        for k in k_range:
            to = other_col(k)
            for q in range(2):
                base = pl.multiple_of((to * 2 + q) * 256, 256)
                x = src[:, pl.ds(base, 256)].astype(BF16)
                outs.append((k, to, q, dot(x, vq[pl.ds(base, 256), :]).astype(BF16)))
        for k, to, q, z in outs:
            if k:
                zs[app, to, q] = z
            else:
                zr[app, col, q] = z
        for k in k_range:
            if k:
                to = other_col(k)
                send(zs.at[app, to], zr.at[app, col], zs_sem.at[app, to], zr_sem.at[app, col], (row, to))

    def put_leaves(at, x):
        turned = pltpu.roll(x, 64, 1)
        zero = jnp.zeros_like(x)
        xlo[at] = jnp.where(low_half, x, zero).astype(BF16)
        xhi[at] = jnp.where(low_half, zero, turned).astype(BF16)
        xlo[at + 1] = jnp.where(low_half, turned, zero).astype(BF16)
        xhi[at + 1] = jnp.where(low_half, zero, x).astype(BF16)

    def spread(src):
        def step(at, _):
            for k in range(4):
                pair = at * 4 + k
                put_leaves(HALO + 2 * pair, src[:, pl.ds(pl.multiple_of(pair * 128, 128), 128)])
            return 0

        lax.fori_loop(0, leaves // 8, step, 0)

    def spread_edges(app):
        for side, inside in ((0, flat > 0), (1, flat < total - 1)):
            arrived(hr.at[app, side], hs_sem.at[app, side], hr_sem.at[app, side])
            for pair in range(HALO // 2):
                x = hr[app, side, :, pair * 128 : (pair + 1) * 128].astype(F32)
                x = jnp.where(inside, x, jnp.zeros_like(x))
                put_leaves(side * (HALO + leaves) + 2 * pair, x)

    def near(dst, first, last):
        def step(at, _):
            for k in range(2):
                pair = at * 2 + k
                parts = []
                for leaf in (2 * pair, 2 * pair + 1):
                    index = [leaf + HALO + off[b, leaf] for b in range(4)]
                    parts.append(
                        jnp.concatenate(
                            [xlo[index[0]] + xhi[index[1]], xlo[index[2]] + xhi[index[3]]], axis=1
                        )
                    )
                lhs = jnp.concatenate(parts, axis=0)
                out = lax.dot_general(
                    lhs, wp[pl.ds(pl.multiple_of(pair * 128, 128), 128), :], NT, preferred_element_type=F32
                )
                dst[:, pl.ds(pl.multiple_of(pair * 128, 128), 128)] = jnp.where(low_half, out[:S], out[S:])
            return 0

        lax.fori_loop(first, last, step, 0)

    def mix_columns(app):
        for k in range(1, n_col):
            source = other_col(k)
            arrived(zr.at[app, source], zs_sem.at[app, source], zr_sem.at[app, source])
        for half in range(2):
            for c in range(n_col // 4):
                tiles = [zr[app, 4 * c + i, half].astype(F32) for i in range(4)]
                for j, tile in enumerate(blocks_swapped(tiles)):
                    zt[4 * half + j, :, 128 * c : 128 * (c + 1)] = tile.astype(BF16)
        for k in list(range(1, n_row)) + [0]:
            j = other_row(k)
            t = dot(zt[j], mc[j]).astype(BF16)
            if k:
                ts[app, j] = t
                send(ts.at[app, j], tr.at[app, row], ts_sem.at[app, j], tr_sem.at[app, row], (j, col))
            else:
                tr[app, row] = t

    def mix_rows(app):
        for k in range(1, n_row):
            source = other_row(k)
            arrived(tr.at[app, source], ts_sem.at[app, source], tr_sem.at[app, source])
        for p in range(n_col // 4):
            for r in range(n_row // 4):
                tiles = [tr[app, 4 * r + i, :, 128 * p : 128 * (p + 1)].astype(F32) for i in range(4)]
                for j, tile in enumerate(blocks_swapped(tiles)):
                    tt[4 * p + j, :, 128 * r : 128 * (r + 1)] = tile.astype(BF16)

    def expand(dst, sums):
        def step(at, carry):
            for k in range(2):
                p = at * 2 + k
                t = dot(tt[p], mr[p])
                high = t.astype(BF16)
                for q in range(2):
                    base = pl.multiple_of((2 * p + q) * 256, 256)
                    weights = uq[pl.ds(pl.multiple_of((2 * p + q) * 128, 128), 128), :]
                    far = dot(high[:, 128 * q : 128 * (q + 1)], weights)
                    for part in range(2):
                        lanes = pl.ds(pl.multiple_of(base + part * 128, 128), 128)
                        out = dst[:, lanes] + far[:, part * 128 : (part + 1) * 128]
                        dst[:, lanes] = out
                        if sums:
                            rx, bx = rv[:, lanes], bv[:, lanes]
                            carry = (carry[0] + rx * out, carry[1] + bx * out, carry[2] + out * out)
            return carry

        zero = jnp.zeros((S, 128), F32)
        return lax.fori_loop(0, n_col // 2, step, (zero, zero, zero) if sums else 0)

    def early_sums():
        def step(at, carry):
            for k in range(4):
                lanes = pl.ds(pl.multiple_of((at * 4 + k) * 128, 128), 128)
                rx, bx = rv[:, lanes], bv[:, lanes]
                carry = (carry[0] + rx * rx, carry[1] + rx * bx, carry[2] + bx * bx)
            return carry

        zero = jnp.zeros((S, 128), F32)
        return lax.fori_loop(0, leaves // 8, step, (zero, zero, zero))

    groups = [list(range(1, 6)), list(range(6, 11)), list(range(11, n_col)) + [0]]

    v_load.wait()
    expand_v()
    r_load.wait()
    pl.semaphore_wait(barrier, len(partners))
    send_edges(0, rv)
    for group in groups:
        compress(0, rv, group)
    spread(rv)
    w_load.wait()
    expand_w(0, leaves // 4)
    spread_edges(0)
    mc_load.wait()
    mix_columns(0)
    u_load.wait()
    expand_u()
    near(bv, 0, leaves // 4)
    mr_load.wait()
    mix_rows(0)
    expand(bv, False)

    send_edges(1, bv)
    for group in groups:
        compress(1, bv, group)
    spread(bv)
    rr, rb, bb = early_sums()
    spread_edges(1)
    near(dv, 0, leaves // 8)
    mix_columns(1)
    near(dv, leaves // 8, leaves // 4)
    mix_rows(1)
    rd, bd, dd = expand(dv, True)

    small = lax.broadcasted_iota(jnp.int32, (8, 128), 1)
    packed = jnp.zeros((8, 128), F32)
    for q, products in enumerate((rr, rb, bb, rd, bd, dd)):
        column = jnp.sum(products, axis=1, keepdims=True)
        for g in range(S // 8):
            packed = jnp.where(small == 8 * g + q, column[8 * g : 8 * (g + 1)], packed)
    g1[...] = packed
    h1[row] = packed
    for k in range(1, n_row):
        to = other_row(k)
        send(g1, h1.at[row], g_sem.at[to], h_sem.at[row], (to, col))
    for k in range(1, n_row):
        source = other_row(k)
        arrived(h1.at[source], g_sem.at[source], h_sem.at[source])
    packed = h1[0]
    for k in range(1, n_row):
        packed = packed + h1[k]
    g2[...] = packed
    h2[col] = packed
    for k in range(1, n_col):
        to = other_col(k)
        send(g2, h2.at[col], g_sem.at[n_row + to], h_sem.at[n_row + col], (row, to))
    for k in range(1, n_col):
        source = other_col(k)
        arrived(h2.at[source], g_sem.at[n_row + source], h_sem.at[n_row + source])
    packed = h2[0]
    for k in range(1, n_col):
        packed = packed + h2[k]

    def of(q):
        return jnp.concatenate([packed[:, 8 * g + q : 8 * g + q + 1] for g in range(S // 8)], axis=0)

    rr, rb, bb, rd, bd, dd = (of(q) for q in range(6))
    inv = 1.0 / rr
    shift = rb * inv
    h21s = bb * inv - shift * shift
    h21 = jnp.sqrt(h21s)
    h11 = 1.0 + shift
    h12 = (rd - shift * rb) * inv / h21
    k22 = (bd - shift * bb - shift * rd + shift * shift * rb) * inv / h21s
    size = (dd - 2.0 * shift * bd + shift * shift * bb) * inv / h21s
    h32s = size - h12 * h12 - k22 * k22
    h22 = 1.0 + k22
    m11 = h11 * h11 + h21s
    m12 = h11 * h12 + h21 * h22
    m22 = h12 * h12 + h22 * h22 + h32s
    det = m11 * m22 - m12 * m12
    y1 = (m22 * h11 - m12 * h12) / det
    y2 = (m11 * h12 - m12 * h11) / det / h21
    wide = lambda x: jnp.broadcast_to(x, (S, 128))
    sol_r, sol_b = wide(y1 - y2 * shift), wide(y2)
    res_r, res_b = wide(1.0 - y1 + y2 * shift), wide(y1 + y2 - y2 * shift)

    def finish(at, _):
        for k in range(4):
            lanes = pl.ds(pl.multiple_of((at * 4 + k) * 128, 128), 128)
            r, b, d = rv[:, lanes], bv[:, lanes], dv[:, lanes]
            sol[:, lanes] = sol_r * r + sol_b * b
            res[:, lanes] = res_r * r - res_b * b - sol_b * d
        return 0

    lax.fori_loop(0, leaves // 8, finish, 0)
    for copy in sends:
        copy.wait_send()


def solution(mesh):
    n_row, n_col = mesh.shape["row"], mesh.shape["col"]

    def body(rhs, near_blocks, near_offsets, v_factor, mix_col, mix_row, u_factor):
        leaves = near_offsets.shape[0]
        unknowns = leaves * LEAF
        w = near_blocks.reshape(leaves, 4, 32, 128).transpose(0, 2, 1, 3).reshape(leaves * 128, 128)
        by_tile = lambda x: x.reshape(leaves // 8, 8, 16, 128).transpose(0, 2, 1, 3).reshape(leaves * 16, 128)
        any_spec = pl.BlockSpec(memory_space=pl.ANY)
        field = pltpu.VMEM((S, unknowns), F32)
        return pl.pallas_call(
            functools.partial(kernel, n_row, n_col),
            out_shape=[jax.ShapeDtypeStruct((S, unknowns), F32)] * 2,
            in_specs=[any_spec, any_spec, pl.BlockSpec(memory_space=pltpu.SMEM)] + [any_spec] * 4,
            out_specs=[pl.BlockSpec(memory_space=pltpu.VMEM)] * 2,
            scratch_shapes=[
                field, field, field,
                pltpu.VMEM((leaves * 128, 128), BF16),
                pltpu.VMEM((leaves * 64, 256), BF16),
                pltpu.VMEM((leaves * 16, 128), BF16),
                pltpu.VMEM((leaves * 64, 128), BF16),
                pltpu.VMEM((leaves * 16, 128), BF16),
                pltpu.VMEM((leaves * 32, 256), BF16),
                pltpu.VMEM(mix_col.shape[1:], BF16),
                pltpu.VMEM(mix_row.shape[1:], BF16),
                pltpu.VMEM((leaves + 2 * HALO, S, 128), BF16),
                pltpu.VMEM((leaves + 2 * HALO, S, 128), BF16),
                pltpu.VMEM((2, 2, S, HALO * LEAF), BF16),
                pltpu.VMEM((2, 2, S, HALO * LEAF), BF16),
                pltpu.VMEM((2, n_col, 2, S, 128), BF16),
                pltpu.VMEM((2, n_col, 2, S, 128), BF16),
                pltpu.VMEM((n_row, S, n_col * RANK), BF16),
                pltpu.VMEM((2, n_row, S, n_col * RANK), BF16),
                pltpu.VMEM((2, n_row, S, n_col * RANK), BF16),
                pltpu.VMEM((n_col, S, n_row * RANK), BF16),
                pltpu.VMEM((4, 128, 128), F32),
                pltpu.VMEM((4, 128, 128), F32),
                pltpu.VMEM((8, 128), F32),
                pltpu.VMEM((n_row, 8, 128), F32),
                pltpu.VMEM((8, 128), F32),
                pltpu.VMEM((n_col, 8, 128), F32),
                pltpu.SemaphoreType.DMA((6,)),
                pltpu.SemaphoreType.DMA((2, 2)),
                pltpu.SemaphoreType.DMA((2, 2)),
                pltpu.SemaphoreType.DMA((2, n_col)),
                pltpu.SemaphoreType.DMA((2, n_col)),
                pltpu.SemaphoreType.DMA((2, n_row)),
                pltpu.SemaphoreType.DMA((2, n_row)),
                pltpu.SemaphoreType.DMA((n_row + n_col,)),
                pltpu.SemaphoreType.DMA((n_row + n_col,)),
            ],
            compiler_params=pltpu.CompilerParams(
                collective_id=0, has_side_effects=True, vmem_limit_bytes=60 * 1024 * 1024
            ),
        )(
            rhs, w, near_offsets.T, by_tile(v_factor),
            mix_col[0], mix_row[0], by_tile(u_factor),
        )

    both = ("row", "col")
    return jax.shard_map(
        body,
        mesh=mesh,
        in_specs=(
            P(None, both),
            P(both, None, None),
            P(both, None),
            P(both, None),
            P("row", "col", None, None),
            P("row", "col", None, None),
            P(both, None),
        ),
        out_specs=(P(None, both), P(None, both)),
        check_vma=False,
    )
```

```python
import functools

import jax
import jax.numpy as jnp
from jax import lax
from jax.experimental import pallas as pl
from jax.experimental.pallas import tpu as pltpu
from jax.sharding import PartitionSpec as P

S = 32
LEAF = 64
RANK = 32
HALO = 4
F32 = jnp.float32
BF16 = jnp.bfloat16
MESH = pl.DeviceIdType.MESH
NT = (((1,), (1,)), ((), ()))


def dot(a, b):
    return jnp.dot(a, b, preferred_element_type=F32)


def lane_index():
    return lax.broadcasted_iota(jnp.int32, (S, 128), 1)


def blocks_swapped(tiles):
    lane = lane_index()
    low_half = lane < 64
    low_quarter = lax.rem(lane, 64) < 32
    a, b, c, d = tiles
    turn = lambda x, by: pltpu.roll(x, by, 1)
    a, c = jnp.where(low_half, a, turn(c, 64)), jnp.where(low_half, turn(a, 64), c)
    b, d = jnp.where(low_half, b, turn(d, 64)), jnp.where(low_half, turn(b, 64), d)
    a, b = jnp.where(low_quarter, a, turn(b, 32)), jnp.where(low_quarter, turn(a, 96), b)
    c, d = jnp.where(low_quarter, c, turn(d, 32)), jnp.where(low_quarter, turn(c, 96), d)
    return a, b, c, d


def kernel(
    n_row, n_col,
    r_hbm, w_hbm, off_hbm, v_hbm, mc_hbm, mr_hbm, u_hbm,
    rv, bv, dv, coefs,
    off, wraw, wp, vraw, vq, uraw, uq, mc, mr, xlo, xhi,
    hs, hr, zs, zr, zt, ts, tr, tt, sa, sb, g1, h1, g2, h2,
    load_sem, hs_sem, hr_sem, zs_sem, zr_sem, ts_sem, tr_sem, g_sem, h_sem,
):
    row = lax.axis_index("row")
    col = lax.axis_index("col")
    flat = row * n_col + col
    total = n_row * n_col
    leaves = off_hbm.shape[1]
    lane = lane_index()
    low_half = lane < 64

    def loads(index, src, dst):
        copy = pltpu.make_async_copy(src, dst, load_sem.at[index])
        copy.start()
        return copy

    v_load = loads(0, v_hbm, vraw)
    r_load = loads(1, r_hbm, rv)
    w_load = loads(2, w_hbm, wraw)
    mc_load = loads(3, mc_hbm, mc)
    mr_load = loads(4, mr_hbm, mr)
    u_load = loads(5, u_hbm, uraw)
    off_load = loads(6, off_hbm, off)

    def other_col(k):
        return lax.rem(col + k, n_col)

    def other_row(k):
        return lax.rem(row + k, n_row)

    def at_flat(k):
        other = lax.rem(flat + k, total)
        return (lax.div(other, n_col), lax.rem(other, n_col))

    up, down = at_flat(1), at_flat(total - 1)
    barrier = pltpu.get_barrier_semaphore()
    partners = [(row, other_col(k)) for k in range(1, n_col)]
    partners += [(other_row(k), col) for k in range(1, n_row)] + [up, down]
    for partner in partners:
        pl.semaphore_signal(barrier, inc=1, device_id=partner, device_id_type=MESH)

    sends = []

    def send(src, dst, send_sem, recv_sem, device):
        copy = pltpu.make_async_remote_copy(
            src_ref=src, dst_ref=dst, send_sem=send_sem, recv_sem=recv_sem,
            device_id=device, device_id_type=MESH,
        )
        copy.start()
        sends.append(copy)

    def arrived(dst, send_sem, recv_sem):
        pltpu.make_async_remote_copy(
            src_ref=dst, dst_ref=dst, send_sem=send_sem, recv_sem=recv_sem,
            device_id=(row, col), device_id_type=MESH,
        ).wait_recv()

    def expand_v():
        group = lax.broadcasted_iota(jnp.int32, (16, 128), 1) // RANK

        def step(at, _):
            for k in range(2):
                one(2 * at + k, k)
            return 0

        def one(at, k):
            sa[k] = vraw[pl.ds(pl.multiple_of(at * 128, 128), 128), :].astype(F32)
            for leaf in range(8):
                j = leaf % 4
                part = sa[k, pl.ds(leaf, 16, stride=8), :]
                for w in range(4):
                    turned = part if j == w else pltpu.roll(part, ((j - w) % 4) * RANK, 1)
                    sb[4 * k + 2 * (leaf // 4) + j // 2, pl.ds((j % 2) * 64 + w, 16, stride=4), :] = jnp.where(
                        group == j, turned, 0.0
                    )
            for q in range(4):
                vq[pl.ds(pl.multiple_of(at * 512 + q * 128, 128), 128), :] = sb[4 * k + q].astype(BF16)

        lax.fori_loop(0, leaves // 16, step, 0)

    def expand_u():
        half = lax.broadcasted_iota(jnp.int32, (16, 128), 1) // LEAF
        nothing = jnp.zeros((64, 128), BF16)

        def step(at, _):
            for k in range(4):
                one(4 * at + k, k)
            return 0

        def one(at, k):
            sa[k] = uraw[pl.ds(pl.multiple_of(at * 128, 128), 128), :].astype(F32)
            for leaf in range(8):
                q = leaf % 4
                part = sa[k, pl.ds(leaf, 16, stride=8), :]
                turned = pltpu.roll(part, 64, 1)
                for w in range(2):
                    sb[2 * k + leaf // 4, pl.ds(q * RANK + w, 16, stride=2), :] = jnp.where(
                        half == q % 2, part if w == q % 2 else turned, 0.0
                    )
            for q in range(2):
                base = pl.multiple_of(at * 256 + q * 128, 128)
                uq[pl.ds(base, 64), 0:128] = sb[2 * k + q, 0:64].astype(BF16)
                uq[pl.ds(base, 64), 128:256] = nothing
                uq[pl.ds(base + 64, 64), 0:128] = nothing
                uq[pl.ds(base + 64, 64), 128:256] = sb[2 * k + q, 64:128].astype(BF16)

        lax.fori_loop(0, leaves // 32, step, 0)

    def expand_w(first, last):
        half = lax.broadcasted_iota(jnp.int32, (32, 128), 1) < 64

        def step(at, _):
            for k in range(8):
                leaf = at * 8 + k
                sa[k] = wraw[pl.ds(pl.multiple_of(leaf * 128, 128), 128), :].astype(F32)
            for k in range(8):
                for b in range(2):
                    one = sa[k, pl.ds(2 * b, 32, stride=4), :]
                    two = sa[k, pl.ds(2 * b + 1, 32, stride=4), :]
                    sb[k, pl.ds(64 * b, 32, stride=2), :] = jnp.where(half, one, pltpu.roll(two, 64, 1))
                    sb[k, pl.ds(64 * b + 1, 32, stride=2), :] = jnp.where(half, pltpu.roll(one, 64, 1), two)
            for k in range(8):
                base = pl.multiple_of((at * 8 + k) * 64, 64)
                wp[pl.ds(base, 64), 0:128] = sb[k, 0:64].astype(BF16)
                wp[pl.ds(base, 64), 128:256] = sb[k, 64:128].astype(BF16)
            return 0

        lax.fori_loop(first, last, step, 0)

    def send_edges(app, src):
        hs[app, 0] = src[:, 0 : HALO * LEAF].astype(BF16)
        hs[app, 1] = src[:, (leaves - HALO) * LEAF : leaves * LEAF].astype(BF16)
        send(hs.at[app, 0], hr.at[app, 1], hs_sem.at[app, 0], hr_sem.at[app, 1], down)
        send(hs.at[app, 1], hr.at[app, 0], hs_sem.at[app, 1], hr_sem.at[app, 0], up)

    def compress(app, src, k_range):
        outs = []
        for k in k_range:
            to = other_col(k)
            for q in range(2):
                base = pl.multiple_of((to * 2 + q) * 256, 256)
                x = src[:, pl.ds(base, 256)].astype(BF16)
                outs.append((k, to, q, dot(x, vq[pl.ds(base, 256), :]).astype(BF16)))
        for k, to, q, z in outs:
            if k:
                zs[app, to, q] = z
            else:
                zr[app, col, q] = z
        for k in k_range:
            if k:
                to = other_col(k)
                send(zs.at[app, to], zr.at[app, col], zs_sem.at[app, to], zr_sem.at[app, col], (row, to))

    def put_leaves(at, x):
        turned = pltpu.roll(x, 64, 1)
        zero = jnp.zeros_like(x)
        xlo[at] = jnp.where(low_half, x, zero).astype(BF16)
        xhi[at] = jnp.where(low_half, zero, turned).astype(BF16)
        xlo[at + 1] = jnp.where(low_half, turned, zero).astype(BF16)
        xhi[at + 1] = jnp.where(low_half, zero, x).astype(BF16)

    def spread(src):
        def step(at, _):
            for k in range(8):
                pair = at * 8 + k
                put_leaves(HALO + 2 * pair, src[:, pl.ds(pl.multiple_of(pair * 128, 128), 128)])
            return 0

        lax.fori_loop(0, leaves // 16, step, 0)

    def spread_edges(app):
        for side, inside in ((0, flat > 0), (1, flat < total - 1)):
            arrived(hr.at[app, side], hs_sem.at[app, side], hr_sem.at[app, side])
            for pair in range(HALO // 2):
                x = hr[app, side, :, pair * 128 : (pair + 1) * 128].astype(F32)
                x = jnp.where(inside, x, jnp.zeros_like(x))
                put_leaves(side * (HALO + leaves) + 2 * pair, x)

    def near(dst, first, last):
        def step(at, _):
            for k in range(8):
                pair = at * 8 + k
                parts = []
                for leaf in (2 * pair, 2 * pair + 1):
                    index = [leaf + HALO + off[b, leaf] for b in range(4)]
                    parts.append(
                        jnp.concatenate(
                            [xlo[index[0]] + xhi[index[1]], xlo[index[2]] + xhi[index[3]]], axis=1
                        )
                    )
                lhs = jnp.concatenate(parts, axis=0)
                out = lax.dot_general(
                    lhs, wp[pl.ds(pl.multiple_of(pair * 128, 128), 128), :], NT, preferred_element_type=F32
                )
                dst[:, pl.ds(pl.multiple_of(pair * 128, 128), 128)] = jnp.where(low_half, out[:S], out[S:])
            return 0

        lax.fori_loop(first, last, step, 0)

    def columns_arrive(app):
        for k in range(1, n_col):
            source = other_col(k)
            arrived(zr.at[app, source], zs_sem.at[app, source], zr_sem.at[app, source])

    def mix_columns(app):
        for half in range(2):
            for c in range(n_col // 4):
                tiles = [zr[app, 4 * c + i, half].astype(F32) for i in range(4)]
                for j, tile in enumerate(blocks_swapped(tiles)):
                    zt[4 * half + j, :, 128 * c : 128 * (c + 1)] = tile.astype(BF16)
        order = list(range(1, n_row)) + [0]
        for first in range(0, n_row, 4):
            ks = order[first : first + 4]
            made = [dot(zt[other_row(k)], mc[other_row(k)]).astype(BF16) for k in ks]
            for k, t in zip(ks, made):
                if k:
                    ts[app, other_row(k)] = t
                else:
                    tr[app, row] = t
            for k in ks:
                j = other_row(k)
                if k:
                    send(ts.at[app, j], tr.at[app, row], ts_sem.at[app, j], tr_sem.at[app, row], (j, col))

    def rows_arrive(app):
        for k in range(1, n_row):
            source = other_row(k)
            arrived(tr.at[app, source], ts_sem.at[app, source], tr_sem.at[app, source])

    def mix_rows(app):
        for p in range(n_col // 4):
            for r in range(n_row // 4):
                tiles = [tr[app, 4 * r + i, :, 128 * p : 128 * (p + 1)].astype(F32) for i in range(4)]
                for j, tile in enumerate(blocks_swapped(tiles)):
                    tt[4 * p + j, :, 128 * r : 128 * (r + 1)] = tile.astype(BF16)

    def expand(dst, sums):
        def step(at, carry):
            ts_ = [dot(tt[at * 8 + k], mr[at * 8 + k]).astype(BF16) for k in range(8)]
            for k, t in enumerate(ts_):
                for q in range(2):
                    quad = (at * 8 + k) * 2 + q
                    base = pl.multiple_of(quad * 256, 256)
                    weights = uq[pl.ds(pl.multiple_of(quad * 128, 128), 128), :]
                    far = dot(t[:, 128 * q : 128 * (q + 1)], weights)
                    for part in range(2):
                        lanes = pl.ds(pl.multiple_of(base + part * 128, 128), 128)
                        out = dst[:, lanes] + far[:, part * 128 : (part + 1) * 128]
                        dst[:, lanes] = out
                        if sums:
                            rx, bx = rv[:, lanes], bv[:, lanes]
                            carry = (carry[0] + rx * out, carry[1] + bx * out, carry[2] + out * out)
            return carry

        zero = jnp.zeros((S, 128), F32)
        return lax.fori_loop(0, n_col // 8, step, (zero, zero, zero) if sums else 0)

    def early_sums():
        def step(at, carry):
            for k in range(4):
                lanes = pl.ds(pl.multiple_of((at * 4 + k) * 128, 128), 128)
                rx, bx = rv[:, lanes], bv[:, lanes]
                carry = (carry[0] + rx * rx, carry[1] + rx * bx, carry[2] + bx * bx)
            return carry

        zero = jnp.zeros((S, 128), F32)
        return lax.fori_loop(0, leaves // 8, step, (zero, zero, zero))

    groups = [list(range(1, 6)), list(range(6, 11)), list(range(11, n_col)) + [0]]

    def at(name):
        return jax.named_scope(name)

    with at("load_v"):
        v_load.wait()
    with at("expand_v"):
        expand_v()
    with at("entry"):
        r_load.wait()
        pl.semaphore_wait(barrier, len(partners))
    with at("z0"):
        send_edges(0, rv)
        for group in groups:
            compress(0, rv, group)
    with at("spread0"):
        spread(rv)
    with at("expand_w"):
        w_load.wait()
        expand_w(0, leaves // 8)
    with at("edges0"):
        spread_edges(0)
    with at("waitcol0"):
        mc_load.wait()
        columns_arrive(0)
    with at("mixcol0"):
        mix_columns(0)
    with at("expand_u"):
        u_load.wait()
        expand_u()
    with at("near0"):
        off_load.wait()
        near(bv, 0, leaves // 16)
    with at("waitrow0"):
        mr_load.wait()
        rows_arrive(0)
    with at("swaprow0"):
        mix_rows(0)
    with at("expand0"):
        expand(bv, False)
    with at("z1"):
        send_edges(1, bv)
        for group in groups:
            compress(1, bv, group)
    with at("spread1"):
        spread(bv)
    with at("sums"):
        rr, rb, bb = early_sums()
    with at("edges1"):
        spread_edges(1)
    with at("near1a"):
        near(dv, 0, leaves // 32)
    with at("waitcol1"):
        columns_arrive(1)
    with at("mixcol1"):
        mix_columns(1)
    with at("near1b"):
        near(dv, leaves // 32, leaves // 16)
    with at("waitrow1"):
        rows_arrive(1)
    with at("swaprow1"):
        mix_rows(1)
    with at("expand1"):
        rd, bd, dd = expand(dv, True)

    with at("reduce"):
        small = lax.broadcasted_iota(jnp.int32, (8, 128), 1)
        packed = jnp.zeros((8, 128), F32)
        for q, products in enumerate((rr, rb, bb, rd, bd, dd)):
            column = jnp.sum(products, axis=1, keepdims=True)
            for g in range(S // 8):
                packed = jnp.where(small == 8 * g + q, column[8 * g : 8 * (g + 1)], packed)
        g1[...] = packed
        h1[row] = packed
        for k in range(1, n_row):
            to = other_row(k)
            send(g1, h1.at[row], g_sem.at[to], h_sem.at[row], (to, col))
        for k in range(1, n_row):
            source = other_row(k)
            arrived(h1.at[source], g_sem.at[source], h_sem.at[source])
        packed = h1[0]
        for k in range(1, n_row):
            packed = packed + h1[k]
        g2[...] = packed
        h2[col] = packed
        for k in range(1, n_col):
            to = other_col(k)
            send(g2, h2.at[col], g_sem.at[n_row + to], h_sem.at[n_row + col], (row, to))
        for k in range(1, n_col):
            source = other_col(k)
            arrived(h2.at[source], g_sem.at[n_row + source], h_sem.at[n_row + source])
        packed = h2[0]
        for k in range(1, n_col):
            packed = packed + h2[k]

    def of(q):
        return jnp.concatenate([packed[:, 8 * g + q : 8 * g + q + 1] for g in range(S // 8)], axis=0)

    with at("coefs"):
        rr, rb, bb, rd, bd, dd = (of(q) for q in range(6))
        inv = 1.0 / rr
        shift = rb * inv
        h21s = bb * inv - shift * shift
        h21 = jnp.sqrt(h21s)
        h11 = 1.0 + shift
        h12 = (rd - shift * rb) * inv / h21
        k22 = (bd - shift * bb - shift * rd + shift * shift * rb) * inv / h21s
        size = (dd - 2.0 * shift * bd + shift * shift * bb) * inv / h21s
        h32s = size - h12 * h12 - k22 * k22
        h22 = 1.0 + k22
        m11 = h11 * h11 + h21s
        m12 = h11 * h12 + h21 * h22
        m22 = h12 * h12 + h22 * h22 + h32s
        det = m11 * m22 - m12 * m12
        y1 = (m22 * h11 - m12 * h12) / det
        y2 = (m11 * h12 - m12 * h11) / det / h21
        for q, x in enumerate((y1 - y2 * shift, y2, 1.0 - y1 + y2 * shift, y1 + y2 - y2 * shift)):
            coefs[q] = jnp.broadcast_to(x, (S, 128))

    with at("drain"):
        for copy in sends:
            copy.wait_send()


def finish(rv, bv, dv, coefs, sol_hbm, res_hbm, sol, res, sem):
    sol_r, sol_b, res_r, res_b = (coefs[q] for q in range(4))
    pieces = sem.shape[1]
    width = rv.shape[1] // pieces
    copies = []
    for piece in range(pieces):
        for at in range(piece * width, (piece + 1) * width, 128):
            lanes = slice(at, at + 128)
            r, b, d = rv[:, lanes], bv[:, lanes], dv[:, lanes]
            sol[:, lanes] = sol_r * r + sol_b * b
            res[:, lanes] = res_r * r - res_b * b - sol_b * d
        lanes = pl.ds(piece * width, width)
        for k, (src, dst) in enumerate(((sol, sol_hbm), (res, res_hbm))):
            copies.append(pltpu.make_async_copy(src.at[:, lanes], dst.at[:, lanes], sem.at[k, piece]))
            copies[-1].start()
    for copy in copies:
        copy.wait()


def solution(mesh):
    n_row, n_col = mesh.shape["row"], mesh.shape["col"]

    def body(rhs, near_blocks, near_offsets, v_factor, mix_col, mix_row, u_factor):
        leaves = near_offsets.shape[0]
        unknowns = leaves * LEAF
        w = near_blocks.reshape(leaves, 4, 32, 128).transpose(0, 2, 1, 3).reshape(leaves * 128, 128)
        by_tile = lambda x: x.reshape(leaves // 8, 8, 16, 128).transpose(0, 2, 1, 3).reshape(leaves * 16, 128)
        any_spec = pl.BlockSpec(memory_space=pl.ANY)
        field = pltpu.VMEM((S, unknowns), F32)
        vmem_spec = pl.BlockSpec(memory_space=pltpu.VMEM)
        parts = pl.pallas_call(
            functools.partial(kernel, n_row, n_col),
            out_shape=[field, field, field, pltpu.VMEM((4, S, 128), F32)],
            in_specs=[pl.BlockSpec(memory_space=pltpu.HBM)] * 7,
            out_specs=[vmem_spec] * 4,
            scratch_shapes=[
                pltpu.SMEM((4, leaves), jnp.int32),
                pltpu.VMEM((leaves * 128, 128), BF16),
                pltpu.VMEM((leaves * 64, 256), BF16),
                pltpu.VMEM((leaves * 16, 128), BF16),
                pltpu.VMEM((leaves * 64, 128), BF16),
                pltpu.VMEM((leaves * 16, 128), BF16),
                pltpu.VMEM((leaves * 32, 256), BF16),
                pltpu.VMEM(mix_col.shape[1:], BF16),
                pltpu.VMEM(mix_row.shape[1:], BF16),
                pltpu.VMEM((leaves + 2 * HALO, S, 128), BF16),
                pltpu.VMEM((leaves + 2 * HALO, S, 128), BF16),
                pltpu.VMEM((2, 2, S, HALO * LEAF), BF16),
                pltpu.VMEM((2, 2, S, HALO * LEAF), BF16),
                pltpu.VMEM((2, n_col, 2, S, 128), BF16),
                pltpu.VMEM((2, n_col, 2, S, 128), BF16),
                pltpu.VMEM((n_row, S, n_col * RANK), BF16),
                pltpu.VMEM((2, n_row, S, n_col * RANK), BF16),
                pltpu.VMEM((2, n_row, S, n_col * RANK), BF16),
                pltpu.VMEM((n_col, S, n_row * RANK), BF16),
                pltpu.VMEM((8, 128, 128), F32),
                pltpu.VMEM((8, 128, 128), F32),
                pltpu.VMEM((8, 128), F32),
                pltpu.VMEM((n_row, 8, 128), F32),
                pltpu.VMEM((8, 128), F32),
                pltpu.VMEM((n_col, 8, 128), F32),
                pltpu.SemaphoreType.DMA((7,)),
                pltpu.SemaphoreType.DMA((2, 2)),
                pltpu.SemaphoreType.DMA((2, 2)),
                pltpu.SemaphoreType.DMA((2, n_col)),
                pltpu.SemaphoreType.DMA((2, n_col)),
                pltpu.SemaphoreType.DMA((2, n_row)),
                pltpu.SemaphoreType.DMA((2, n_row)),
                pltpu.SemaphoreType.DMA((n_row + n_col,)),
                pltpu.SemaphoreType.DMA((n_row + n_col,)),
            ],
            compiler_params=pltpu.CompilerParams(
                collective_id=0, has_side_effects=True, vmem_limit_bytes=54 * 1024 * 1024
            ),
        )(
            rhs, w, near_offsets.T, by_tile(v_factor),
            mix_col[0], mix_row[0], by_tile(u_factor),
        )
        return pl.pallas_call(
            finish,
            out_shape=[jax.ShapeDtypeStruct((S, unknowns), F32)] * 2,
            in_specs=[vmem_spec] * 4,
            out_specs=[any_spec] * 2,
            scratch_shapes=[
                pltpu.VMEM((S, unknowns), F32),
                pltpu.VMEM((S, unknowns), F32),
                pltpu.SemaphoreType.DMA((2, 4)),
            ],
            compiler_params=pltpu.CompilerParams(vmem_limit_bytes=8 * 1024 * 1024),
        )(*(pltpu.with_memory_space_constraint(x, pltpu.VMEM) for x in parts))

    both = ("row", "col")
    return jax.shard_map(
        body,
        mesh=mesh,
        in_specs=(
            P(None, both),
            P(both, None, None),
            P(both, None),
            P(both, None),
            P("row", "col", None, None),
            P("row", "col", None, None),
            P(both, None),
        ),
        out_specs=(P(None, both), P(None, both)),
        check_vma=False,
    )
```

```python
import functools

import jax
import jax.numpy as jnp
from jax import lax
from jax.experimental import pallas as pl
from jax.experimental.pallas import tpu as pltpu
from jax.sharding import PartitionSpec as P

S = 32
LEAF = 64
RANK = 32
HALO = 4
F32 = jnp.float32
BF16 = jnp.bfloat16
MESH = pl.DeviceIdType.MESH
NT = (((1,), (1,)), ((), ()))


def dot(a, b):
    return jnp.dot(a, b, preferred_element_type=F32)


def lane_index():
    return lax.broadcasted_iota(jnp.int32, (S, 128), 1)


def blocks_swapped(tiles):
    lane = lane_index()
    low_half = lane < 64
    low_quarter = lax.rem(lane, 64) < 32
    a, b, c, d = tiles
    turn = lambda x, by: pltpu.roll(x, by, 1)
    a, c = jnp.where(low_half, a, turn(c, 64)), jnp.where(low_half, turn(a, 64), c)
    b, d = jnp.where(low_half, b, turn(d, 64)), jnp.where(low_half, turn(b, 64), d)
    a, b = jnp.where(low_quarter, a, turn(b, 32)), jnp.where(low_quarter, turn(a, 96), b)
    c, d = jnp.where(low_quarter, c, turn(d, 32)), jnp.where(low_quarter, turn(c, 96), d)
    return a, b, c, d


def kernel(
    n_row, n_col,
    r_hbm, w_hbm, off_hbm, v_hbm, mc_hbm, mr_hbm, u_hbm,
    rv, bv, dv, coefs,
    off, wraw, wp, vraw, vq, uraw, uq, mc, mr, xd, turn,
    hs, hr, zs, zr, zt, ts, tr, tt, t2, sv, sa, sb, g1, h1, g2, h2,
    load_sem, sent, hr_sem, zr_sem, tr_sem, h_sem,
):
    row = lax.axis_index("row")
    col = lax.axis_index("col")
    flat = row * n_col + col
    total = n_row * n_col
    leaves = off_hbm.shape[1]
    lane = lane_index()
    low_half = lane < 64

    def loads(index, src, dst):
        copy = pltpu.make_async_copy(src, dst, load_sem.at[index])
        copy.start()
        return copy

    col_slow, col_fast, row_fast = lax.div(col, 4), lax.rem(col, 4), lax.rem(row, 4)
    home = lax.div(row, 4)
    away = 1 - home
    steps = [(z, y) for z in range(4) for y in range(4)]
    steps.sort(key=lambda d: -min(d[0], 4 - d[0]) - min(d[1], 4 - d[1]))
    order = [4 * lax.rem(col_slow + z, 4) + lax.rem(col_fast + y, 4) for z, y in steps]
    own = order[-1]
    inner = leaves // 2 - 16

    def at_half(half):
        return 0 if half is away else 1


    for group in range(4):
        for to in order[4 * group : 4 * (group + 1)]:
            rows = pl.ds(pl.multiple_of(to * 128, 128), 128)
            pltpu.make_async_copy(v_hbm.at[rows], vraw.at[rows], load_sem.at[5 + 2 * group]).start()
            lanes = pl.ds(pl.multiple_of(to * 512, 512), 512)
            pltpu.make_async_copy(r_hbm.at[:, lanes], rv.at[:, lanes], load_sem.at[6 + 2 * group]).start()
    off_load = loads(0, off_hbm, off)
    w_load = loads(1, w_hbm, wraw)

    def first_loads(group):
        pltpu.make_async_copy(v_hbm.at[0:512], vraw.at[0:512], load_sem.at[5 + 2 * group]).wait()
        pltpu.make_async_copy(r_hbm.at[:, 0:2048], rv.at[:, 0:2048], load_sem.at[6 + 2 * group]).wait()

    def other_col(k):
        return lax.rem(col + k, n_col)

    def other_row(k):
        return lax.rem(row + k, n_row)

    def at_flat(k):
        other = lax.rem(flat + k, total)
        return (lax.div(other, n_col), lax.rem(other, n_col))

    up, down = at_flat(1), at_flat(total - 1)
    barrier = pltpu.get_barrier_semaphore()
    partners = [(row, other_col(k)) for k in range(1, n_col)]
    partners += [(other_row(k), col) for k in range(1, n_row)] + [up, down]
    for partner in partners:
        pl.semaphore_signal(barrier, inc=1, device_id=partner, device_id_type=MESH)

    def send(src, dst, send_sem, recv_sem, device):
        pltpu.make_async_remote_copy(
            src_ref=src, dst_ref=dst, send_sem=send_sem, recv_sem=recv_sem,
            device_id=device, device_id_type=MESH,
        ).start()

    def arrived(all_of_them, recv_sem):
        pltpu.make_async_copy(all_of_them, all_of_them, recv_sem).wait()

    def set_turn():
        m = lax.broadcasted_iota(jnp.int32, (256, 256), 0)
        n = lax.broadcasted_iota(jnp.int32, (256, 256), 1)
        source = (n // 64) * 64 + 4 * lax.rem(n, 16) + lax.rem(n, 64) // 16
        turn[...] = jnp.where(m == source, 1.0, 0.0).astype(BF16)

    def expand_v(to, half):
        group = lax.broadcasted_iota(jnp.int32, (16, 128), 1) // RANK
        base = pl.multiple_of(to * 128, 128)
        pieces = []
        for j in range(4):
            part = sv[pl.ds(base + 4 * half + j, 16, stride=8), :].astype(BF16)
            for w in range(4):
                turned = part if j == w else pltpu.roll(part, ((j - w) % 4) * RANK, 1)
                pieces.append(jnp.where(group == j, turned, jnp.zeros_like(turned)))
        expanded = jnp.concatenate(pieces, axis=0)
        vq[pl.ds(pl.multiple_of((2 * to + half) * 256, 256), 256), :] = expanded
        return expanded

    def expand_u():
        half = lax.broadcasted_iota(jnp.int32, (16, 128), 1) // LEAF
        nothing = jnp.zeros((64, 128), BF16)

        def step(at, _):
            for k in range(8):
                one(8 * at + k, k)
            return 0

        def one(at, k):
            sa[k] = uraw[pl.ds(pl.multiple_of(at * 128, 128), 128), :].astype(F32)
            for leaf in range(8):
                q = leaf % 4
                part = sa[k, pl.ds(leaf, 16, stride=8), :]
                turned = pltpu.roll(part, 64, 1)
                for w in range(2):
                    sb[2 * k + leaf // 4, pl.ds(q * RANK + w, 16, stride=2), :] = jnp.where(
                        half == q % 2, part if w == q % 2 else turned, 0.0
                    )
            for q in range(2):
                base = pl.multiple_of(at * 256 + q * 128, 128)
                uq[pl.ds(base, 64), 0:128] = sb[2 * k + q, 0:64].astype(BF16)
                uq[pl.ds(base, 64), 128:256] = nothing
                uq[pl.ds(base + 64, 64), 0:128] = nothing
                uq[pl.ds(base + 64, 64), 128:256] = sb[2 * k + q, 64:128].astype(BF16)

        lax.fori_loop(0, leaves // 64, step, 0)

    def expand_w(first, last):
        half = lax.broadcasted_iota(jnp.int32, (32, 128), 1) < 64

        def step(at, _):
            for k in range(16):
                leaf = at * 16 + k
                sa[k] = wraw[pl.ds(pl.multiple_of(leaf * 128, 128), 128), :].astype(F32)
            for k in range(16):
                for b in range(2):
                    one = sa[k, pl.ds(2 * b, 32, stride=4), :]
                    two = sa[k, pl.ds(2 * b + 1, 32, stride=4), :]
                    sb[k, pl.ds(64 * b, 32, stride=2), :] = jnp.where(half, one, pltpu.roll(two, 64, 1))
                    sb[k, pl.ds(64 * b + 1, 32, stride=2), :] = jnp.where(half, pltpu.roll(one, 64, 1), two)
            for k in range(16):
                base = pl.multiple_of((at * 16 + k) * 64, 64)
                wp[pl.ds(base, 64), 0:128] = sb[k, 0:64].astype(BF16)
                wp[pl.ds(base, 64), 128:256] = sb[k, 64:128].astype(BF16)
            return 0

        lax.fori_loop(first, last, step, 0)

    def send_edges(app, src):
        hs[app, 0] = src[:, 0 : HALO * LEAF].astype(BF16)
        hs[app, 1] = src[:, (leaves - HALO) * LEAF : leaves * LEAF].astype(BF16)
        send(hs.at[app, 0], hr.at[app, 1], sent.at[0], hr_sem.at[app], down)
        send(hs.at[app, 1], hr.at[app, 0], sent.at[0], hr_sem.at[app], up)

    def turned_fields(values):
        x = jnp.concatenate([x.astype(BF16) for x in values], axis=0)
        x = dot(x, turn[...]).astype(BF16)
        return [x[S * k : S * (k + 1)] for k in range(len(values))]

    def compress(app, half, tos, fields, factors):
        made = [dot(x, v).astype(BF16) for x, v in zip(fields, factors)]
        for to, z in zip(tos, made):
            if to is own:
                zr[app, half, col] = z
            else:
                zs[app, half, to] = z
        for to in tos:
            if to is not own:
                send(
                    zs.at[app, half, to], zr.at[app, half, col],
                    sent.at[1], zr_sem.at[app, at_half(half)], (row, to),
                )

    def quad(to, half):
        return pl.ds(pl.multiple_of((2 * to + half) * 256, 256), 256)

    def grouped(size):
        return [(half, order[at : at + size]) for half in (away, home) for at in range(0, n_col, size)]

    def first_compress(ready, others):
        waiting = None
        for at, group in enumerate(grouped(4) + [None]):
            made = None
            if at == 4:
                others()
            if group is not None:
                half, tos = group
                if half is away:
                    first_loads(at)
                for to in tos:
                    if half is away:
                        rows = pl.ds(pl.multiple_of(to * 128, 128), 128)
                        sv[rows, :] = vraw[rows, :].astype(F32)
                factors = [expand_v(to, half) for to in tos]
                made = (half, tos, turned_fields([rv[:, quad(to, half)] for to in tos]), factors)
            if waiting is not None:
                ready()
                compress(0, *waiting)
            waiting = made

    def expand_and_compress(app, dst):
        added = turned = None
        for group in grouped(8) + [None, None]:
            next_added = next_turned = None
            if group is not None:
                next_added = (*group, far_added(dst, *group))
            if added is not None:
                half, tos, values = added
                next_turned = (half, tos, turned_fields(values), [vq[quad(to, half), :] for to in tos])
            if turned is not None:
                compress(app + 1, *turned)
            added, turned = next_added, next_turned

    def far_added(dst, half, tos):
        fars = [
            dot(t2[half, to], uq[pl.ds(pl.multiple_of((2 * to + half) * 128, 128), 128), :]) for to in tos
        ]
        outs = []
        for to, far in zip(tos, fars):
            lanes = quad(to, half)
            out = dst[:, lanes] + far
            dst[:, lanes] = out
            outs.append(out)
        return outs

    def put_leaves(at, x):
        turned = pltpu.roll(x, 64, 1)
        xd[at] = jnp.where(low_half, x, turned)
        xd[at + 1] = jnp.where(low_half, turned, x)

    def spread(src):
        def step(at, _):
            for k in range(32):
                pair = at * 32 + k
                put_leaves(HALO + 2 * pair, src[:, pl.ds(pl.multiple_of(pair * 128, 128), 128)].astype(BF16))
            return 0

        lax.fori_loop(0, leaves // 64, step, 0)

    def spread_edges(app):
        arrived(hr.at[app], hr_sem.at[app])
        for side, inside in ((0, flat > 0), (1, flat < total - 1)):
            for pair in range(HALO // 2):
                x = hr[app, side, :, pair * 128 : (pair + 1) * 128]
                x = jnp.where(inside, x, jnp.zeros_like(x))
                put_leaves(side * (HALO + leaves) + 2 * pair, x)

    def near_pairs(dst, pairs):
        for pair in pairs:
            parts = []
            for leaf in (2 * pair, 2 * pair + 1):
                index = [leaf + HALO + off[b, leaf] for b in range(4)]
                parts.append(
                    jnp.concatenate(
                        [
                            jnp.where(low_half, xd[index[0]], xd[index[1]]),
                            jnp.where(low_half, xd[index[2]], xd[index[3]]),
                        ],
                        axis=1,
                    )
                )
            lhs = jnp.concatenate(parts, axis=0)
            rows = pl.ds(pair * 128 if isinstance(pair, int) else pl.multiple_of(pair * 128, 128), 128)
            out = lax.dot_general(lhs, wp[rows, :], NT, preferred_element_type=F32)
            dst[:, rows] = jnp.where(low_half, out[:S], out[S:])

    def near(dst, first, count):
        def step(at, _):
            near_pairs(dst, [first + at * 16 + k for k in range(16)])
            return 0

        lax.fori_loop(0, count // 16, step, 0)

    def near_edges(dst):
        near_pairs(dst, list(range(8)) + [leaves // 2 - 8 + j for j in range(8)])

    def columns(app, half):
        arrived(zr.at[app, 0, pl.ds(0, n_col - 1)], zr_sem.at[app, at_half(half)])
        for c in range(4):
            tiles = [zr[app, half, 4 * c + i] for i in range(4)]
            for j, tile in enumerate(blocks_swapped(tiles)):
                zt[4 * half + j, c] = tile

    def mix_columns(app, half):
        to_rows = [4 * half + lax.rem(row_fast + k, 4) for k in (1, 2, 3, 0)]
        made = []
        for j in to_rows:
            z = jnp.concatenate([zt[j, c] for c in range(4)], axis=1)
            made.append(dot(z, mc[j]).astype(BF16))
        for at, (j, t) in enumerate(zip(to_rows, made)):
            stays = half is home and at == 3
            for p in range(4):
                if stays:
                    tr[app, row, p] = t[:, 128 * p : 128 * (p + 1)]
                else:
                    ts[app, j, p] = t[:, 128 * p : 128 * (p + 1)]
        for at, j in enumerate(to_rows):
            if not (half is home and at == 3):
                send(
                    ts.at[app, j], tr.at[app, row],
                    sent.at[2], tr_sem.at[app, at_half(half)], (j, col),
                )

    def rows(app, half):
        arrived(tr.at[app, pl.ds(0, 4 if half is away else 3)], tr_sem.at[app, at_half(half)])
        for p in range(4):
            tiles = [tr[app, 4 * half + i, p] for i in range(4)]
            for j, tile in enumerate(blocks_swapped(tiles)):
                tt[4 * p + j, half] = tile

    def mix_rows(app):
        for at in range(0, n_col, 8):
            made = [
                dot(jnp.concatenate([tt[p, 0], tt[p, 1]], axis=1), mr[p]).astype(BF16) for p in range(at, at + 8)
            ]
            for p, t in zip(range(at, at + 8), made):
                t2[0, p] = t[:, 0:128]
                t2[1, p] = t[:, 128:256]

    def last_expand(dst):
        zero = jnp.zeros((S, 128), F32)
        rd, bd, dd = zero, zero, zero
        for at in range(0, 2 * n_col, 8):
            fars = [dot(t2[k % 2, k // 2], uq[128 * k : 128 * (k + 1), :]) for k in range(at, at + 8)]
            for k, far in zip(range(at, at + 8), fars):
                for part in range(2):
                    lanes = slice(256 * k + 128 * part, 256 * k + 128 * (part + 1))
                    out = dst[:, lanes] + far[:, 128 * part : 128 * (part + 1)]
                    dst[:, lanes] = out
                    rd, bd, dd = rd + rv[:, lanes] * out, bd + bv[:, lanes] * out, dd + out * out
        return rd, bd, dd

    def placed(packed, qs, sums):
        small = lax.broadcasted_iota(jnp.int32, (8, 128), 1)
        for q, products in zip(qs, sums):
            column = jnp.sum(products, axis=1, keepdims=True)
            for g in range(S // 8):
                packed = jnp.where(small == 8 * g + q, column[8 * g : 8 * (g + 1)], packed)
        return packed

    def early_sums():
        def step(at, carry):
            for k in range(16):
                lanes = pl.ds(pl.multiple_of((at * 16 + k) * 128, 128), 128)
                rx, bx = rv[:, lanes], bv[:, lanes]
                carry = (carry[0] + rx * rx, carry[1] + rx * bx, carry[2] + bx * bx)
            return carry

        zero = jnp.zeros((S, 128), F32)
        return lax.fori_loop(0, leaves // 32, step, (zero, zero, zero))

    def at(name):
        return jax.named_scope(name)

    set_turn()
    met = []

    def meet():
        if not met:
            pl.semaphore_wait(barrier, len(partners))
            met.append(True)

    later = []

    def others():
        for at, (src, dst) in enumerate(((mc_hbm, mc), (u_hbm, uraw), (mr_hbm, mr))):
            later.append(loads(2 + at, src, dst))

    with at("z0"):
        first_compress(meet, others)
        mc_load, u_load, mr_load = later
        send_edges(0, rv)
    with at("spread0"):
        spread(rv)
    with at("expand_w"):
        w_load.wait()
        expand_w(0, leaves // 16)
    mc_load.wait()
    with at("colA0"):
        columns(0, away)
    with at("mixA0"):
        mix_columns(0, away)
    with at("colB0"):
        columns(0, home)
    with at("mixB0"):
        mix_columns(0, home)
    with at("expand_u"):
        u_load.wait()
        expand_u()
    with at("near0"):
        off_load.wait()
        near(bv, 8, inner)
    with at("edges0"):
        spread_edges(0)
        near_edges(bv)
    with at("rowA0"):
        rows(0, away)
    with at("rowB0"):
        rows(0, home)
    with at("mixrow0"):
        mr_load.wait()
        mix_rows(0)
    with at("expz0"):
        expand_and_compress(0, bv)
        send_edges(1, bv)
    with at("spread1"):
        spread(bv)
    with at("sums"):
        packed = placed(jnp.zeros((8, 128), F32), (0, 1, 2), early_sums())
    with at("near1a"):
        near(dv, 8, 16)
    with at("colA1"):
        columns(1, away)
    with at("mixA1"):
        mix_columns(1, away)
    with at("colB1"):
        columns(1, home)
    with at("mixB1"):
        mix_columns(1, home)
    with at("near1b"):
        near(dv, 24, inner - 16)
    with at("edges1"):
        spread_edges(1)
        near_edges(dv)
    with at("rowA1"):
        rows(1, away)
    with at("rowB1"):
        rows(1, home)
    with at("mixrow1"):
        mix_rows(1)
    with at("expand1"):
        rd, bd, dd = last_expand(dv)

    with at("reduce"):
        packed = placed(packed, (3, 4, 5), (rd, bd, dd))
        g1[...] = packed
        h1[row] = packed
        for k in range(1, n_row):
            to = other_row(k)
            send(g1, h1.at[row], sent.at[3], h_sem.at[0], (to, col))
        arrived(h1.at[pl.ds(0, n_row - 1)], h_sem.at[0])
        packed = h1[0]
        for k in range(1, n_row):
            packed = packed + h1[k]
        g2[...] = packed
        h2[col] = packed
        for k in range(1, n_col):
            to = other_col(k)
            send(g2, h2.at[col], sent.at[4], h_sem.at[1], (row, to))
        arrived(h2.at[pl.ds(0, n_col - 1)], h_sem.at[1])
        packed = h2[0]
        for k in range(1, n_col):
            packed = packed + h2[k]

    with at("coefs"):
        rr, rb, bb, rd, bd, dd = (packed if q == 0 else pltpu.roll(packed, 128 - q, 1) for q in range(6))
        inv = 1.0 / rr
        shift = rb * inv
        h21s = bb * inv - shift * shift
        inv_h21s = 1.0 / h21s
        h21 = jnp.sqrt(h21s)
        inv_h21 = h21 * inv_h21s
        h11 = 1.0 + shift
        h12 = (rd - shift * rb) * (inv * inv_h21)
        k22 = (bd - shift * (bb + rd - shift * rb)) * (inv * inv_h21s)
        size = (dd - shift * (2.0 * bd - shift * bb)) * (inv * inv_h21s)
        h32s = size - h12 * h12 - k22 * k22
        h22 = 1.0 + k22
        m11 = h11 * h11 + h21s
        m12 = h11 * h12 + h21 * h22
        m22 = h12 * h12 + h22 * h22 + h32s
        inv_det = 1.0 / (m11 * m22 - m12 * m12)
        y1 = (m22 * h11 - m12 * h12) * inv_det
        y2 = (m11 * h12 - m12 * h11) * inv_det * inv_h21
        for q, x in enumerate((y1 - y2 * shift, y2, 1.0 - y1 + y2 * shift, y1 + y2 - y2 * shift)):
            for g in range(S // 8):
                coefs[q, 8 * g : 8 * (g + 1)] = jnp.broadcast_to(x[:, 8 * g : 8 * g + 1], (8, 128))

    with at("drain"):
        arrived(hs, sent.at[0])
        arrived(zs.at[:, :, pl.ds(0, n_col - 1)], sent.at[1])
        arrived(ts.at[:, pl.ds(0, n_row - 1)], sent.at[2])
        arrived(h1.at[pl.ds(0, n_row - 1)], sent.at[3])
        arrived(h2.at[pl.ds(0, n_col - 1)], sent.at[4])


def finish(rv, bv, dv, coefs, sol_hbm, res_hbm, sol, res, sem):
    sol_r, sol_b, res_r, res_b = (coefs[q] for q in range(4))
    pieces = sem.shape[1]
    width = rv.shape[1] // pieces
    copies = []
    for piece in range(pieces):
        for at in range(piece * width, (piece + 1) * width, 128):
            lanes = slice(at, at + 128)
            r, b, d = rv[:, lanes], bv[:, lanes], dv[:, lanes]
            sol[:, lanes] = sol_r * r + sol_b * b
            res[:, lanes] = res_r * r - res_b * b - sol_b * d
        lanes = pl.ds(piece * width, width)
        for k, (src, dst) in enumerate(((sol, sol_hbm), (res, res_hbm))):
            copies.append(pltpu.make_async_copy(src.at[:, lanes], dst.at[:, lanes], sem.at[k, piece]))
            copies[-1].start()
    for copy in copies:
        copy.wait()


def solution(mesh):
    n_row, n_col = mesh.shape["row"], mesh.shape["col"]

    def body(rhs, near_blocks, near_offsets, v_factor, mix_col, mix_row, u_factor):
        leaves = near_offsets.shape[0]
        unknowns = leaves * LEAF
        w = near_blocks.reshape(leaves, 4, 32, 128).transpose(0, 2, 1, 3).reshape(leaves * 128, 128)
        by_tile = lambda x: x.reshape(leaves // 8, 8, 16, 128).transpose(0, 2, 1, 3).reshape(leaves * 16, 128)
        any_spec = pl.BlockSpec(memory_space=pl.ANY)
        field = pltpu.VMEM((S, unknowns), F32)
        vmem_spec = pl.BlockSpec(memory_space=pltpu.VMEM)
        parts = pl.pallas_call(
            functools.partial(kernel, n_row, n_col),
            out_shape=[field, field, field, pltpu.VMEM((4, S, 128), F32)],
            in_specs=[pl.BlockSpec(memory_space=pltpu.HBM)] * 7,
            out_specs=[vmem_spec] * 4,
            scratch_shapes=[
                pltpu.SMEM((4, leaves), jnp.int32),
                pltpu.VMEM((leaves * 128, 128), BF16),
                pltpu.VMEM((leaves * 64, 256), BF16),
                pltpu.VMEM((leaves * 16, 128), BF16),
                pltpu.VMEM((leaves * 64, 128), BF16),
                pltpu.VMEM((leaves * 16, 128), BF16),
                pltpu.VMEM((leaves * 32, 256), BF16),
                pltpu.VMEM(mix_col.shape[1:], BF16),
                pltpu.VMEM(mix_row.shape[1:], BF16),
                pltpu.VMEM((leaves + 2 * HALO, S, 128), BF16),
                pltpu.VMEM((256, 256), BF16),
                pltpu.VMEM((2, 2, S, HALO * LEAF), BF16),
                pltpu.VMEM((2, 2, S, HALO * LEAF), BF16),
                pltpu.VMEM((2, 2, n_col, S, 128), BF16),
                pltpu.VMEM((2, 2, n_col, S, 128), BF16),
                pltpu.VMEM((n_row, 4, S, 128), BF16),
                pltpu.VMEM((2, n_row, 4, S, 128), BF16),
                pltpu.VMEM((2, n_row, 4, S, 128), BF16),
                pltpu.VMEM((n_col, 2, S, 128), BF16),
                pltpu.VMEM((2, n_col, S, 128), BF16),
                pltpu.VMEM((leaves * 16, 128), F32),
                pltpu.VMEM((16, 128, 128), F32),
                pltpu.VMEM((16, 128, 128), F32),
                pltpu.VMEM((8, 128), F32),
                pltpu.VMEM((n_row, 8, 128), F32),
                pltpu.VMEM((8, 128), F32),
                pltpu.VMEM((n_col, 8, 128), F32),
                pltpu.SemaphoreType.DMA((5 + 2 * 4,)),
                pltpu.SemaphoreType.DMA((5,)),
                pltpu.SemaphoreType.DMA((2,)),
                pltpu.SemaphoreType.DMA((2, 2)),
                pltpu.SemaphoreType.DMA((2, 2)),
                pltpu.SemaphoreType.DMA((2,)),
            ],
            compiler_params=pltpu.CompilerParams(
                collective_id=0, has_side_effects=True, vmem_limit_bytes=54 * 1024 * 1024
            ),
        )(
            rhs, w, near_offsets.T, by_tile(v_factor),
            mix_col[0], mix_row[0], by_tile(u_factor),
        )
        return pl.pallas_call(
            finish,
            out_shape=[jax.ShapeDtypeStruct((S, unknowns), F32)] * 2,
            in_specs=[vmem_spec] * 4,
            out_specs=[any_spec] * 2,
            scratch_shapes=[
                pltpu.VMEM((S, unknowns), F32),
                pltpu.VMEM((S, unknowns), F32),
                pltpu.SemaphoreType.DMA((2, 4)),
            ],
            compiler_params=pltpu.CompilerParams(vmem_limit_bytes=8 * 1024 * 1024),
        )(*(pltpu.with_memory_space_constraint(x, pltpu.VMEM) for x in parts))

    both = ("row", "col")
    return jax.shard_map(
        body,
        mesh=mesh,
        in_specs=(
            P(None, both),
            P(both, None, None),
            P(both, None),
            P(both, None),
            P("row", "col", None, None),
            P("row", "col", None, None),
            P(both, None),
        ),
        out_specs=(P(None, both), P(None, both)),
        check_vma=False,
    )
```

```python
import functools

import jax
import jax.numpy as jnp
from jax import lax
from jax.experimental import pallas as pl
from jax.experimental.pallas import tpu as pltpu
from jax.sharding import PartitionSpec as P

S = 32
LEAF = 64
RANK = 32
HALO = 4
F32 = jnp.float32
BF16 = jnp.bfloat16
MESH = pl.DeviceIdType.MESH
NT = (((1,), (1,)), ((), ()))


def dot(a, b):
    return jnp.dot(a, b, preferred_element_type=F32)


def lane_index():
    return lax.broadcasted_iota(jnp.int32, (S, 128), 1)


def blocks_swapped(tiles):
    lane = lane_index()
    low_half = lane < 64
    low_quarter = lax.rem(lane, 64) < 32
    a, b, c, d = tiles
    turn = lambda x, by: pltpu.roll(x, by, 1)
    a, c = jnp.where(low_half, a, turn(c, 64)), jnp.where(low_half, turn(a, 64), c)
    b, d = jnp.where(low_half, b, turn(d, 64)), jnp.where(low_half, turn(b, 64), d)
    a, b = jnp.where(low_quarter, a, turn(b, 32)), jnp.where(low_quarter, turn(a, 96), b)
    c, d = jnp.where(low_quarter, c, turn(d, 32)), jnp.where(low_quarter, turn(c, 96), d)
    return a, b, c, d


def kernel(
    n_row, n_col,
    r_hbm, w_hbm, off_hbm, v_hbm, mc_hbm, mr_hbm, u_hbm,
    rv, bv, dv, coefs,
    off, wraw, wp, vraw, vq, uraw, uq, mc, mr, xd, turn,
    hs, hr, zs, zr, zt, ts, tr, tt, tp, t2, sv, sa, sb, g1, h1, g2, h2,
    load_sem, sent, hr_sem, zr_sem, tr_sem, h_sem,
):
    row = lax.axis_index("row")
    col = lax.axis_index("col")
    flat = row * n_col + col
    total = n_row * n_col
    leaves = off_hbm.shape[1]
    lane = lane_index()
    low_half = lane < 64

    def loads(index, src, dst):
        copy = pltpu.make_async_copy(src, dst, load_sem.at[index])
        copy.start()
        return copy

    col_slow, col_fast, row_fast = lax.div(col, 4), lax.rem(col, 4), lax.rem(row, 4)
    home = lax.rem(lax.div(row, 2), 2)
    away = 1 - home

    def slot_of(half, i):
        return 2 * half + (i % 2) + 4 * (i // 2)

    steps = [(z, y) for z in range(4) for y in range(4)]
    steps.sort(key=lambda d: -min(d[0], 4 - d[0]) - min(d[1], 4 - d[1]))
    order = [4 * lax.rem(col_slow + z, 4) + lax.rem(col_fast + y, 4) for z, y in steps]
    own = order[-1]
    inner = leaves // 2 - 16

    def at_half(half):
        return 0 if half is home else 1

    for group in range(4):
        for k in range(4 * group, 4 * (group + 1)):
            to = order[k]
            rows = pl.ds(pl.multiple_of(to * 128, 128), 128)
            place = vraw.at[pl.ds(128 * k, 128)]
            pltpu.make_async_copy(v_hbm.at[rows], place, load_sem.at[5 + 2 * group]).start()
            lanes = pl.ds(pl.multiple_of(to * 512, 512), 512)
            pltpu.make_async_copy(r_hbm.at[:, lanes], rv.at[:, lanes], load_sem.at[6 + 2 * group]).start()
    off_load = loads(0, off_hbm, off)
    w_load = loads(1, w_hbm, wraw)

    def first_loads(group):
        pltpu.make_async_copy(v_hbm.at[0:512], vraw.at[0:512], load_sem.at[5 + 2 * group]).wait()
        pltpu.make_async_copy(r_hbm.at[:, 0:2048], rv.at[:, 0:2048], load_sem.at[6 + 2 * group]).wait()

    def other_col(k):
        return lax.rem(col + k, n_col)

    def other_row(k):
        return lax.rem(row + k, n_row)

    def at_flat(k):
        other = lax.rem(flat + k, total)
        return (lax.div(other, n_col), lax.rem(other, n_col))

    up, down = at_flat(1), at_flat(total - 1)
    barrier = pltpu.get_barrier_semaphore()
    partners = [(row, other_col(k)) for k in range(1, n_col)]
    partners += [(other_row(k), col) for k in range(1, n_row)] + [up, down]
    for partner in partners:
        pl.semaphore_signal(barrier, inc=1, device_id=partner, device_id_type=MESH)

    def send(src, dst, send_sem, recv_sem, device):
        pltpu.make_async_remote_copy(
            src_ref=src, dst_ref=dst, send_sem=send_sem, recv_sem=recv_sem,
            device_id=device, device_id_type=MESH,
        ).start()

    def arrived(all_of_them, recv_sem):
        pltpu.make_async_copy(all_of_them, all_of_them, recv_sem).wait()

    def set_turn():
        m = lax.broadcasted_iota(jnp.int32, (256, 256), 0)
        n = lax.broadcasted_iota(jnp.int32, (256, 256), 1)
        source = (n // 64) * 64 + 4 * lax.rem(n, 16) + lax.rem(n, 64) // 16
        turn[...] = jnp.where(m == source, 1.0, 0.0).astype(BF16)

    def expand_v(k, half):
        group = lax.broadcasted_iota(jnp.int32, (16, 128), 1) // RANK
        pieces = []
        for j in range(4):
            part = sv[k, pl.ds(slot_of(half, j), 16, stride=8), :].astype(BF16)
            for w in range(4):
                turned = part if j == w else pltpu.roll(part, ((j - w) % 4) * RANK, 1)
                pieces.append(jnp.where(group == j, turned, jnp.zeros_like(turned)))
        vq[at_half(half), k] = jnp.concatenate(pieces, axis=0)

    def expand_u():
        half = lax.broadcasted_iota(jnp.int32, (16, 128), 1) // LEAF
        nothing = jnp.zeros((64, 128), BF16)

        def step(at, _):
            for k in range(8):
                one(8 * at + k, k)
            return 0

        def one(at, k):
            sa[k] = uraw[pl.ds(pl.multiple_of(at * 128, 128), 128), :].astype(F32)
            for leaf in range(8):
                half_at, q = (leaf // 2) % 2, leaf % 2 + 2 * (leaf // 4)
                part = sa[k, pl.ds(leaf, 16, stride=8), :]
                turned = pltpu.roll(part, 64, 1)
                for w in range(2):
                    sb[2 * k + half_at, pl.ds(q * RANK + w, 16, stride=2), :] = jnp.where(
                        half == q % 2, part if w == q % 2 else turned, 0.0
                    )
            for q in range(2):
                base = pl.multiple_of(at * 256 + q * 128, 128)
                uq[pl.ds(base, 64), 0:128] = sb[2 * k + q, 0:64].astype(BF16)
                uq[pl.ds(base, 64), 128:256] = nothing
                uq[pl.ds(base + 64, 64), 0:128] = nothing
                uq[pl.ds(base + 64, 64), 128:256] = sb[2 * k + q, 64:128].astype(BF16)

        lax.fori_loop(0, leaves // 64, step, 0)

    def expand_w(first, last):
        half = lax.broadcasted_iota(jnp.int32, (32, 128), 1) < 64

        def step(at, _):
            for k in range(16):
                leaf = at * 16 + k
                sa[k] = wraw[pl.ds(pl.multiple_of(leaf * 128, 128), 128), :].astype(F32)
            for k in range(16):
                for b in range(2):
                    one = sa[k, pl.ds(2 * b, 32, stride=4), :]
                    two = sa[k, pl.ds(2 * b + 1, 32, stride=4), :]
                    sb[k, pl.ds(64 * b, 32, stride=2), :] = jnp.where(half, one, pltpu.roll(two, 64, 1))
                    sb[k, pl.ds(64 * b + 1, 32, stride=2), :] = jnp.where(half, pltpu.roll(one, 64, 1), two)
            for k in range(16):
                base = pl.multiple_of((at * 16 + k) * 64, 64)
                wp[pl.ds(base, 64), 0:128] = sb[k, 0:64].astype(BF16)
                wp[pl.ds(base, 64), 128:256] = sb[k, 64:128].astype(BF16)
            return 0

        lax.fori_loop(first, last, step, 0)

    def send_edges(app, src):
        hs[app, 0] = src[:, 0 : HALO * LEAF].astype(BF16)
        hs[app, 1] = src[:, (leaves - HALO) * LEAF : leaves * LEAF].astype(BF16)
        send(hs.at[app, 0], hr.at[app, 1], sent.at[0], hr_sem.at[app], down)
        send(hs.at[app, 1], hr.at[app, 0], sent.at[0], hr_sem.at[app], up)

    def field(src, to, half):
        return jnp.concatenate([src[:, lanes] for lanes in tiles_of(to, half)], axis=1)

    def turned_fields(values):
        x = jnp.concatenate([x.astype(BF16) for x in values], axis=0)
        x = dot(x, turn[...]).astype(BF16)
        return [x[S * k : S * (k + 1)] for k in range(len(values))]

    def compress(app, half, ks, fields):
        h = at_half(half)
        made = [dot(x, vq[h, k]).astype(BF16) for k, x in zip(ks, fields)]
        for k, z in zip(ks, made):
            if k == n_col - 1:
                zr[app, half, col] = z
            else:
                zs[app, h, k] = z
        for k in ks:
            if k < n_col - 1:
                send(zs.at[app, h, k], zr.at[app, half, col], sent.at[1], zr_sem.at[app, h], (row, order[k]))

    def tiles_of(to, half):
        return [pl.ds(pl.multiple_of(to * 512 + half * 128 + part * 256, 128), 128) for part in range(2)]

    def first_compress(ready, others):
        ks = list(range(n_col))
        for half in (home, away):
            if half is home:
                for group in range(4):
                    first_loads(group)
                    for k in range(4 * group, 4 * group + 4):
                        sv[k] = vraw[128 * k : 128 * (k + 1), :].astype(F32)
            for k in ks:
                expand_v(k, half)
            fields = turned_fields([field(rv, to, half) for to in order])
            if half is home:
                ready()
            compress(0, half, ks, fields)
            if half is home:
                others()

    def expand_and_compress(app, dst):
        for half in (home, away):
            fields = turned_fields(far_added(dst, half, order))
            compress(app + 1, half, list(range(n_col)), fields)

    def far_added(dst, half, tos):
        fars = [
            dot(t2[half, to], uq[pl.ds(pl.multiple_of((2 * to + half) * 128, 128), 128), :]) for to in tos
        ]
        old = [field(dst, to, half) for to in tos]
        outs = [x + far for x, far in zip(old, fars)]
        for to, out in zip(tos, outs):
            for part, lanes in enumerate(tiles_of(to, half)):
                dst[:, lanes] = out[:, 128 * part : 128 * (part + 1)]
        return outs

    def put_leaves(at, x):
        turned = pltpu.roll(x, 64, 1)
        xd[at] = jnp.where(low_half, x, turned)
        xd[at + 1] = jnp.where(low_half, turned, x)

    def spread(src):
        def step(at, _):
            for k in range(32):
                pair = at * 32 + k
                put_leaves(HALO + 2 * pair, src[:, pl.ds(pl.multiple_of(pair * 128, 128), 128)].astype(BF16))
            return 0

        lax.fori_loop(0, leaves // 64, step, 0)

    def spread_edges(app):
        arrived(hr.at[app], hr_sem.at[app])
        for side, inside in ((0, flat > 0), (1, flat < total - 1)):
            for pair in range(HALO // 2):
                x = hr[app, side, :, pair * 128 : (pair + 1) * 128]
                x = jnp.where(inside, x, jnp.zeros_like(x))
                put_leaves(side * (HALO + leaves) + 2 * pair, x)

    def near_pairs(dst, pairs):
        for pair in pairs:
            parts = []
            for leaf in (2 * pair, 2 * pair + 1):
                index = [leaf + HALO + off[b, leaf] for b in range(4)]
                parts.append(
                    jnp.concatenate(
                        [
                            jnp.where(low_half, xd[index[0]], xd[index[1]]),
                            jnp.where(low_half, xd[index[2]], xd[index[3]]),
                        ],
                        axis=1,
                    )
                )
            lhs = jnp.concatenate(parts, axis=0)
            rows = pl.ds(pair * 128 if isinstance(pair, int) else pl.multiple_of(pair * 128, 128), 128)
            out = lax.dot_general(lhs, wp[rows, :], NT, preferred_element_type=F32)
            dst[:, rows] = jnp.where(low_half, out[:S], out[S:])

    def near(dst, first, count):
        def step(at, _):
            near_pairs(dst, [first + at * 16 + k for k in range(16)])
            return 0

        lax.fori_loop(0, count // 16, step, 0)

    def near_edges(dst):
        near_pairs(dst, list(range(8)) + [leaves // 2 - 8 + j for j in range(8)])

    def columns(app, half):
        arrived(zr.at[app, 0, pl.ds(0, n_col - 1)], zr_sem.at[app, at_half(half)])
        for c in range(4):
            tiles = [zr[app, half, 4 * c + i] for i in range(4)]
            for j, tile in enumerate(blocks_swapped(tiles)):
                zt[slot_of(half, j), c] = tile

    def mix_columns(app, half):
        to_rows = [2 * half + lax.rem(lax.rem(row, 2) + k, 2) + 4 * lax.rem(lax.div(row, 4) + m, 2) for m, k in ((1, 0), (1, 1), (0, 1), (0, 0))]
        made = []
        for j in to_rows:
            z = jnp.concatenate([zt[j, c] for c in range(4)], axis=1)
            made.append(dot(z, mc[j]).astype(BF16))
        for at, (j, t) in enumerate(zip(to_rows, made)):
            stays = half is home and at == 3
            for p in range(4):
                if stays:
                    tr[app, row, p] = t[:, 128 * p : 128 * (p + 1)]
                else:
                    ts[app, j, p] = t[:, 128 * p : 128 * (p + 1)]
            if not stays:
                send(ts.at[app, j], tr.at[app, row], sent.at[2], tr_sem.at[app, at_half(half)], (j, col))

    def rows(app, half):
        arrived(tr.at[app, pl.ds(0, 4 if half is away else 3)], tr_sem.at[app, at_half(half)])
        for p in range(4):
            tiles = [tr[app, slot_of(half, i), p] for i in range(4)]
            for j, tile in enumerate(blocks_swapped(tiles)):
                tt[4 * p + j, half] = tile

    def part_of_rows(p, half):
        weights = [mr[p, pl.ds(pl.multiple_of(64 * half + 128 * i, 64), 64), :] for i in range(2)]
        return dot(tt[p, half], jnp.concatenate(weights, axis=0))

    def mix_rows_first(half):
        for at in range(0, n_col, 8):
            for p in range(at, at + 8):
                tp[p] = part_of_rows(p, half)

    def mix_rows(half):
        for at in range(0, n_col, 8):
            made = [(tp[p] + part_of_rows(p, half)).astype(BF16) for p in range(at, at + 8)]
            for p, t in zip(range(at, at + 8), made):
                one, two = t[:, 0:128], t[:, 128:256]
                t2[0, p] = jnp.where(low_half, one, pltpu.roll(two, 64, 1))
                t2[1, p] = jnp.where(low_half, pltpu.roll(one, 64, 1), two)

    def last_expand(dst):
        zero = jnp.zeros((S, 128), F32)
        rd, bd, dd = zero, zero, zero
        for at in range(0, 2 * n_col, 8):
            fars = [dot(t2[k % 2, k // 2], uq[128 * k : 128 * (k + 1), :]) for k in range(at, at + 8)]
            for k, far in zip(range(at, at + 8), fars):
                for part in range(2):
                    base = 512 * (k // 2) + 128 * (k % 2) + 256 * part
                    lanes = slice(base, base + 128)
                    out = dst[:, lanes] + far[:, 128 * part : 128 * (part + 1)]
                    dst[:, lanes] = out
                    rd, bd, dd = rd + rv[:, lanes] * out, bd + bv[:, lanes] * out, dd + out * out
        return rd, bd, dd

    def placed(packed, qs, sums):
        small = lax.broadcasted_iota(jnp.int32, (8, 128), 1)
        for q, products in zip(qs, sums):
            column = jnp.sum(products, axis=1, keepdims=True)
            for g in range(S // 8):
                packed = jnp.where(small == 8 * g + q, column[8 * g : 8 * (g + 1)], packed)
        return packed

    def early_sums():
        def step(at, carry):
            for k in range(16):
                lanes = pl.ds(pl.multiple_of((at * 16 + k) * 128, 128), 128)
                rx, bx = rv[:, lanes], bv[:, lanes]
                carry = (carry[0] + rx * rx, carry[1] + rx * bx, carry[2] + bx * bx)
            return carry

        zero = jnp.zeros((S, 128), F32)
        return lax.fori_loop(0, leaves // 32, step, (zero, zero, zero))

    def at(name):
        return jax.named_scope(name)

    set_turn()
    met = []

    def meet():
        if not met:
            pl.semaphore_wait(barrier, len(partners))
            met.append(True)

    later = []

    def others():
        for at, (src, dst) in enumerate(((mc_hbm, mc), (u_hbm, uraw), (mr_hbm, mr))):
            later.append(loads(2 + at, src, dst))

    with at("z0"):
        first_compress(meet, others)
        mc_load, u_load, mr_load = later
        send_edges(0, rv)
    with at("spread0"):
        spread(rv)
    with at("expand_w"):
        w_load.wait()
        expand_w(0, leaves // 16)
    mc_load.wait()
    with at("colA0"):
        columns(0, home)
    with at("mixA0"):
        mix_columns(0, home)
    with at("colB0"):
        columns(0, away)
    with at("mixB0"):
        mix_columns(0, away)
    with at("expand_u"):
        u_load.wait()
        expand_u()
    with at("near0"):
        off_load.wait()
        near(bv, 8, inner)
    with at("edges0"):
        spread_edges(0)
        near_edges(bv)
    with at("rowA0"):
        rows(0, home)
        mr_load.wait()
        mix_rows_first(home)
    with at("rowB0"):
        rows(0, away)
    with at("mixrow0"):
        mix_rows(away)
    with at("expz0"):
        expand_and_compress(0, bv)
        send_edges(1, bv)
    with at("spread1"):
        spread(bv)
    with at("sums"):
        packed = placed(jnp.zeros((8, 128), F32), (0, 1, 2), early_sums())
    with at("near1a"):
        near(dv, 8, 16)
    with at("colA1"):
        columns(1, home)
    with at("mixA1"):
        mix_columns(1, home)
    with at("colB1"):
        columns(1, away)
    with at("mixB1"):
        mix_columns(1, away)
    with at("near1b"):
        near(dv, 24, inner - 16)
    with at("edges1"):
        spread_edges(1)
        near_edges(dv)
    with at("rowA1"):
        rows(1, home)
        mix_rows_first(home)
    with at("rowB1"):
        rows(1, away)
    with at("mixrow1"):
        mix_rows(away)
    with at("expand1"):
        rd, bd, dd = last_expand(dv)

    with at("reduce"):
        packed = placed(packed, (3, 4, 5), (rd, bd, dd))
        g1[...] = packed
        h1[row] = packed
        for k in range(1, n_row):
            to = other_row(k)
            send(g1, h1.at[row], sent.at[3], h_sem.at[0], (to, col))
        with at("red1"):
            arrived(h1.at[pl.ds(0, n_row - 1)], h_sem.at[0])
        packed = h1[0]
        for k in range(1, n_row):
            packed = packed + h1[k]
        g2[...] = packed
        h2[col] = packed
        for k in range(1, n_col):
            send(g2, h2.at[col], sent.at[4], h_sem.at[1], (row, other_col(k)))
        with at("red2"):
            arrived(h2.at[pl.ds(0, n_col - 1)], h_sem.at[1])
        packed = h2[0]
        for k in range(1, n_col):
            packed = packed + h2[k]

    with at("coefs"):
        rr, rb, bb, rd, bd, dd = (packed if q == 0 else pltpu.roll(packed, 128 - q, 1) for q in range(6))
        inv = 1.0 / rr
        shift = rb * inv
        h21s = bb * inv - shift * shift
        inv_h21s = 1.0 / h21s
        h21 = jnp.sqrt(h21s)
        inv_h21 = h21 * inv_h21s
        h11 = 1.0 + shift
        h12 = (rd - shift * rb) * (inv * inv_h21)
        k22 = (bd - shift * (bb + rd - shift * rb)) * (inv * inv_h21s)
        size = (dd - shift * (2.0 * bd - shift * bb)) * (inv * inv_h21s)
        h32s = size - h12 * h12 - k22 * k22
        h22 = 1.0 + k22
        m11 = h11 * h11 + h21s
        m12 = h11 * h12 + h21 * h22
        m22 = h12 * h12 + h22 * h22 + h32s
        inv_det = 1.0 / (m11 * m22 - m12 * m12)
        y1 = (m22 * h11 - m12 * h12) * inv_det
        y2 = (m11 * h12 - m12 * h11) * inv_det * inv_h21
        for q, x in enumerate((y1 - y2 * shift, y2, 1.0 - y1 + y2 * shift, y1 + y2 - y2 * shift)):
            for g in range(S // 8):
                coefs[q, 8 * g : 8 * (g + 1)] = jnp.broadcast_to(x[:, 8 * g : 8 * g + 1], (8, 128))

    with at("drain"):
        arrived(hs, sent.at[0])
        arrived(zs.at[:, :, pl.ds(0, n_col - 1)], sent.at[1])
        arrived(ts.at[:, pl.ds(0, n_row - 1)], sent.at[2])
        arrived(h1.at[pl.ds(0, n_row - 1)], sent.at[3])
        arrived(h2.at[pl.ds(0, n_col - 1)], sent.at[4])


def finish(rv, bv, dv, coefs, sol_hbm, res_hbm, sol, res, sem):
    copies = []
    for g in range(S // 8):
        rows = slice(8 * g, 8 * (g + 1))
        sol_r, sol_b, res_r, res_b = (coefs[q, rows] for q in range(4))
        for at in range(0, rv.shape[1], 128):
            lanes = slice(at, at + 128)
            r, b, d = rv[rows, lanes], bv[rows, lanes], dv[rows, lanes]
            sol[rows, lanes] = sol_r * r + sol_b * b
            res[rows, lanes] = res_r * r - res_b * b - sol_b * d
        for k, (src, dst) in enumerate(((sol, sol_hbm), (res, res_hbm))):
            copies.append(pltpu.make_async_copy(src.at[rows], dst.at[rows], sem.at[k, g]))
            copies[-1].start()
    for copy in copies:
        copy.wait()


def solution(mesh):
    n_row, n_col = mesh.shape["row"], mesh.shape["col"]

    def body(rhs, near_blocks, near_offsets, v_factor, mix_col, mix_row, u_factor):
        leaves = near_offsets.shape[0]
        unknowns = leaves * LEAF
        w = near_blocks.reshape(leaves, 4, 32, 128).transpose(0, 2, 1, 3).reshape(leaves * 128, 128)
        by_tile = lambda x: x.reshape(leaves // 8, 8, 16, 128).transpose(0, 2, 1, 3).reshape(leaves * 16, 128)
        any_spec = pl.BlockSpec(memory_space=pl.ANY)
        field = pltpu.VMEM((S, unknowns), F32)
        vmem_spec = pl.BlockSpec(memory_space=pltpu.VMEM)
        parts = pl.pallas_call(
            functools.partial(kernel, n_row, n_col),
            out_shape=[field, field, field, pltpu.VMEM((4, S, 128), F32)],
            in_specs=[pl.BlockSpec(memory_space=pltpu.HBM)] * 7,
            out_specs=[vmem_spec] * 4,
            scratch_shapes=[
                pltpu.SMEM((4, leaves), jnp.int32),
                pltpu.VMEM((leaves * 128, 128), BF16),
                pltpu.VMEM((leaves * 64, 256), BF16),
                pltpu.VMEM((leaves * 16, 128), BF16),
                pltpu.VMEM((2, n_col, 256, 128), BF16),
                pltpu.VMEM((leaves * 16, 128), BF16),
                pltpu.VMEM((leaves * 32, 256), BF16),
                pltpu.VMEM(mix_col.shape[1:], BF16),
                pltpu.VMEM(mix_row.shape[1:], BF16),
                pltpu.VMEM((leaves + 2 * HALO, S, 128), BF16),
                pltpu.VMEM((256, 256), BF16),
                pltpu.VMEM((2, 2, S, HALO * LEAF), BF16),
                pltpu.VMEM((2, 2, S, HALO * LEAF), BF16),
                pltpu.VMEM((2, 2, n_col, S, 128), BF16),
                pltpu.VMEM((2, 2, n_col, S, 128), BF16),
                pltpu.VMEM((n_row, 4, S, 128), BF16),
                pltpu.VMEM((2, n_row, 4, S, 128), BF16),
                pltpu.VMEM((2, n_row, 4, S, 128), BF16),
                pltpu.VMEM((n_col, 2, S, 128), BF16),
                pltpu.VMEM((n_col, S, n_row * RANK), F32),
                pltpu.VMEM((2, n_col, S, 128), BF16),
                pltpu.VMEM((n_col, 128, 128), F32),
                pltpu.VMEM((16, 128, 128), F32),
                pltpu.VMEM((16, 128, 128), F32),
                pltpu.VMEM((8, 128), F32),
                pltpu.VMEM((n_row, 8, 128), F32),
                pltpu.VMEM((8, 128), F32),
                pltpu.VMEM((n_col, 8, 128), F32),
                pltpu.SemaphoreType.DMA((5 + 2 * 4,)),
                pltpu.SemaphoreType.DMA((5,)),
                pltpu.SemaphoreType.DMA((2,)),
                pltpu.SemaphoreType.DMA((2, 2)),
                pltpu.SemaphoreType.DMA((2, 2)),
                pltpu.SemaphoreType.DMA((2,)),
            ],
            compiler_params=pltpu.CompilerParams(
                collective_id=0, has_side_effects=True, vmem_limit_bytes=54 * 1024 * 1024
            ),
        )(
            rhs, w, near_offsets.T, by_tile(v_factor),
            mix_col[0], mix_row[0], by_tile(u_factor),
        )
        return pl.pallas_call(
            finish,
            out_shape=[jax.ShapeDtypeStruct((S, unknowns), F32)] * 2,
            in_specs=[vmem_spec] * 4,
            out_specs=[any_spec] * 2,
            scratch_shapes=[
                pltpu.VMEM((S, unknowns), F32),
                pltpu.VMEM((S, unknowns), F32),
                pltpu.SemaphoreType.DMA((2, S // 8)),
            ],
            compiler_params=pltpu.CompilerParams(vmem_limit_bytes=8 * 1024 * 1024),
        )(*(pltpu.with_memory_space_constraint(x, pltpu.VMEM) for x in parts))

    both = ("row", "col")
    return jax.shard_map(
        body,
        mesh=mesh,
        in_specs=(
            P(None, both),
            P(both, None, None),
            P(both, None),
            P(both, None),
            P("row", "col", None, None),
            P("row", "col", None, None),
            P(both, None),
        ),
        out_specs=(P(None, both), P(None, both)),
        check_vma=False,
    )
```

```python
import functools

import jax
import jax.numpy as jnp
from jax import lax
from jax.experimental import pallas as pl
from jax.experimental.pallas import tpu as pltpu
from jax.sharding import PartitionSpec as P

S = 32
LEAF = 64
RANK = 32
HALO = 4
F32 = jnp.float32
BF16 = jnp.bfloat16
MESH = pl.DeviceIdType.MESH
NT = (((1,), (1,)), ((), ()))


def dot(a, b):
    return jnp.dot(a, b, preferred_element_type=F32)


def lane_index():
    return lax.broadcasted_iota(jnp.int32, (S, 128), 1)


def blocks_swapped(tiles):
    lane = lane_index()
    low_half = lane < 64
    low_quarter = lax.rem(lane, 64) < 32
    a, b, c, d = tiles
    turn = lambda x, by: pltpu.roll(x, by, 1)
    a, c = jnp.where(low_half, a, turn(c, 64)), jnp.where(low_half, turn(a, 64), c)
    b, d = jnp.where(low_half, b, turn(d, 64)), jnp.where(low_half, turn(b, 64), d)
    a, b = jnp.where(low_quarter, a, turn(b, 32)), jnp.where(low_quarter, turn(a, 96), b)
    c, d = jnp.where(low_quarter, c, turn(d, 32)), jnp.where(low_quarter, turn(c, 96), d)
    return a, b, c, d


def kernel(
    n_row, n_col,
    r_hbm, w_hbm, off_hbm, v_hbm, mc_hbm, mr_hbm, u_hbm,
    rv, bv, dv, coefs,
    off, wraw, wp, vraw, vq, uraw, uq, mc, mr, xd, turn,
    hs, hr, zs, zr, zt, ts, tr, tt, tp, t2, sv, sa, sb, g, h,
    load_sem, sent, hr_sem, zr_sem, tr_sem, h_sem,
):
    row = lax.axis_index("row")
    col = lax.axis_index("col")
    flat = row * n_col + col
    total = n_row * n_col
    leaves = off_hbm.shape[1]
    lane = lane_index()
    low_half = lane < 64

    def loads(index, src, dst):
        copy = pltpu.make_async_copy(src, dst, load_sem.at[index])
        copy.start()
        return copy

    col_slow, col_fast, row_fast = lax.div(col, 4), lax.rem(col, 4), lax.rem(row, 4)
    home = lax.rem(lax.div(row, 2), 2)
    away = 1 - home

    def slot_of(half, i):
        return 2 * half + (i % 2) + 4 * (i // 2)

    steps = [(z, y) for z in range(4) for y in range(4)]
    steps.sort(key=lambda d: -min(d[0], 4 - d[0]) - min(d[1], 4 - d[1]))
    order = [4 * lax.rem(col_slow + z, 4) + lax.rem(col_fast + y, 4) for z, y in steps]
    own = order[-1]
    inner = leaves // 2 - 16

    def at_half(half):
        return 0 if half is home else 1

    for group in range(4):
        for k in range(4 * group, 4 * (group + 1)):
            to = order[k]
            rows = pl.ds(pl.multiple_of(to * 128, 128), 128)
            place = vraw.at[pl.ds(128 * k, 128)]
            pltpu.make_async_copy(v_hbm.at[rows], place, load_sem.at[5 + 2 * group]).start()
            lanes = pl.ds(pl.multiple_of(to * 512, 512), 512)
            pltpu.make_async_copy(r_hbm.at[:, lanes], rv.at[:, lanes], load_sem.at[6 + 2 * group]).start()
    off_load = loads(0, off_hbm, off)
    w_load = loads(1, w_hbm, wraw)

    def first_loads(group):
        pltpu.make_async_copy(v_hbm.at[0:512], vraw.at[0:512], load_sem.at[5 + 2 * group]).wait()
        pltpu.make_async_copy(r_hbm.at[:, 0:2048], rv.at[:, 0:2048], load_sem.at[6 + 2 * group]).wait()

    def other_col(k):
        return lax.rem(col + k, n_col)

    def other_row(k):
        return lax.rem(row + k, n_row)

    def at_flat(k):
        other = lax.rem(flat + k, total)
        return (lax.div(other, n_col), lax.rem(other, n_col))

    up, down = at_flat(1), at_flat(total - 1)
    barrier = pltpu.get_barrier_semaphore()
    partners = [(row, other_col(k)) for k in range(1, n_col)]
    partners += [(other_row(k), col) for k in range(1, n_row)] + [up, down]
    for partner in partners:
        pl.semaphore_signal(barrier, inc=1, device_id=partner, device_id_type=MESH)

    def send(src, dst, send_sem, recv_sem, device):
        pltpu.make_async_remote_copy(
            src_ref=src, dst_ref=dst, send_sem=send_sem, recv_sem=recv_sem,
            device_id=device, device_id_type=MESH,
        ).start()

    def arrived(all_of_them, recv_sem):
        pltpu.make_async_copy(all_of_them, all_of_them, recv_sem).wait()

    def set_turn():
        m = lax.broadcasted_iota(jnp.int32, (256, 256), 0)
        n = lax.broadcasted_iota(jnp.int32, (256, 256), 1)
        source = (n // 64) * 64 + 4 * lax.rem(n, 16) + lax.rem(n, 64) // 16
        turn[...] = jnp.where(m == source, 1.0, 0.0).astype(BF16)

    def expand_v(k, half):
        group = lax.broadcasted_iota(jnp.int32, (16, 128), 1) // RANK
        pieces = []
        for j in range(4):
            part = sv[k, pl.ds(slot_of(half, j), 16, stride=8), :].astype(BF16)
            for w in range(4):
                turned = part if j == w else pltpu.roll(part, ((j - w) % 4) * RANK, 1)
                pieces.append(jnp.where(group == j, turned, jnp.zeros_like(turned)))
        vq[at_half(half), k] = jnp.concatenate(pieces, axis=0)

    def expand_u():
        half = lax.broadcasted_iota(jnp.int32, (16, 128), 1) // LEAF
        nothing = jnp.zeros((64, 128), BF16)

        def step(at, _):
            for k in range(8):
                one(8 * at + k, k)
            return 0

        def one(at, k):
            sa[k] = uraw[pl.ds(pl.multiple_of(at * 128, 128), 128), :].astype(F32)
            for leaf in range(8):
                half_at, q = (leaf // 2) % 2, leaf % 2 + 2 * (leaf // 4)
                part = sa[k, pl.ds(leaf, 16, stride=8), :]
                turned = pltpu.roll(part, 64, 1)
                for w in range(2):
                    sb[2 * k + half_at, pl.ds(q * RANK + w, 16, stride=2), :] = jnp.where(
                        half == q % 2, part if w == q % 2 else turned, 0.0
                    )
            for q in range(2):
                base = pl.multiple_of(at * 256 + q * 128, 128)
                uq[pl.ds(base, 64), 0:128] = sb[2 * k + q, 0:64].astype(BF16)
                uq[pl.ds(base, 64), 128:256] = nothing
                uq[pl.ds(base + 64, 64), 0:128] = nothing
                uq[pl.ds(base + 64, 64), 128:256] = sb[2 * k + q, 64:128].astype(BF16)

        lax.fori_loop(0, leaves // 64, step, 0)

    def expand_w(first, last):
        half = lax.broadcasted_iota(jnp.int32, (32, 128), 1) < 64

        def step(at, _):
            for k in range(16):
                leaf = at * 16 + k
                sa[k] = wraw[pl.ds(pl.multiple_of(leaf * 128, 128), 128), :].astype(F32)
            for k in range(16):
                for b in range(2):
                    one = sa[k, pl.ds(2 * b, 32, stride=4), :]
                    two = sa[k, pl.ds(2 * b + 1, 32, stride=4), :]
                    sb[k, pl.ds(64 * b, 32, stride=2), :] = jnp.where(half, one, pltpu.roll(two, 64, 1))
                    sb[k, pl.ds(64 * b + 1, 32, stride=2), :] = jnp.where(half, pltpu.roll(one, 64, 1), two)
            for k in range(16):
                base = pl.multiple_of((at * 16 + k) * 64, 64)
                wp[pl.ds(base, 64), 0:128] = sb[k, 0:64].astype(BF16)
                wp[pl.ds(base, 64), 128:256] = sb[k, 64:128].astype(BF16)
            return 0

        lax.fori_loop(first, last, step, 0)

    def send_edges(app, src):
        hs[app, 0] = src[:, 0 : HALO * LEAF].astype(BF16)
        hs[app, 1] = src[:, (leaves - HALO) * LEAF : leaves * LEAF].astype(BF16)
        send(hs.at[app, 0], hr.at[app, 1], sent.at[0], hr_sem.at[app], down)
        send(hs.at[app, 1], hr.at[app, 0], sent.at[0], hr_sem.at[app], up)

    def field(src, to, half):
        return jnp.concatenate([src[:, lanes] for lanes in tiles_of(to, half)], axis=1)

    def turned_fields(values):
        x = jnp.concatenate([x.astype(BF16) for x in values], axis=0)
        x = dot(x, turn[...]).astype(BF16)
        return [x[S * k : S * (k + 1)] for k in range(len(values))]

    def compress(app, half, ks, fields):
        h = at_half(half)
        made = [dot(x, vq[h, k]).astype(BF16) for k, x in zip(ks, fields)]
        for k, z in zip(ks, made):
            if k == n_col - 1:
                zr[app, half, col] = z
            else:
                zs[app, h, k] = z
        for k in ks:
            if k < n_col - 1:
                send(zs.at[app, h, k], zr.at[app, half, col], sent.at[1], zr_sem.at[app, h], (row, order[k]))

    def tiles_of(to, half):
        return [pl.ds(pl.multiple_of(to * 512 + half * 128 + part * 256, 128), 128) for part in range(2)]

    def first_compress(ready, others):
        ks = list(range(n_col))
        for half in (home, away):
            if half is home:
                for group in range(4):
                    first_loads(group)
                    for k in range(4 * group, 4 * group + 4):
                        sv[k] = vraw[128 * k : 128 * (k + 1), :].astype(F32)
            for k in ks:
                expand_v(k, half)
            fields = turned_fields([field(rv, to, half) for to in order])
            if half is home:
                ready()
            compress(0, half, ks, fields)
            if half is home:
                others()

    def expand_and_compress(app, dst):
        for half in (home, away):
            fields = turned_fields(far_added(dst, half, order))
            compress(app + 1, half, list(range(n_col)), fields)

    def far_added(dst, half, tos):
        fars = [
            dot(t2[half, to], uq[pl.ds(pl.multiple_of((2 * to + half) * 128, 128), 128), :]) for to in tos
        ]
        old = [field(dst, to, half) for to in tos]
        outs = [x + far for x, far in zip(old, fars)]
        for to, out in zip(tos, outs):
            for part, lanes in enumerate(tiles_of(to, half)):
                dst[:, lanes] = out[:, 128 * part : 128 * (part + 1)]
        return outs

    def put_leaves(at, x):
        turned = pltpu.roll(x, 64, 1)
        xd[at] = jnp.where(low_half, x, turned)
        xd[at + 1] = jnp.where(low_half, turned, x)

    def spread(src):
        def step(at, _):
            for k in range(32):
                pair = at * 32 + k
                put_leaves(HALO + 2 * pair, src[:, pl.ds(pl.multiple_of(pair * 128, 128), 128)].astype(BF16))
            return 0

        lax.fori_loop(0, leaves // 64, step, 0)

    def spread_edges(app):
        arrived(hr.at[app], hr_sem.at[app])
        for side, inside in ((0, flat > 0), (1, flat < total - 1)):
            for pair in range(HALO // 2):
                x = hr[app, side, :, pair * 128 : (pair + 1) * 128]
                x = jnp.where(inside, x, jnp.zeros_like(x))
                put_leaves(side * (HALO + leaves) + 2 * pair, x)

    def near_pairs(dst, pairs):
        for pair in pairs:
            parts = []
            for leaf in (2 * pair, 2 * pair + 1):
                index = [leaf + HALO + off[b, leaf] for b in range(4)]
                parts.append(
                    jnp.concatenate(
                        [
                            jnp.where(low_half, xd[index[0]], xd[index[1]]),
                            jnp.where(low_half, xd[index[2]], xd[index[3]]),
                        ],
                        axis=1,
                    )
                )
            lhs = jnp.concatenate(parts, axis=0)
            rows = pl.ds(pair * 128 if isinstance(pair, int) else pl.multiple_of(pair * 128, 128), 128)
            out = lax.dot_general(lhs, wp[rows, :], NT, preferred_element_type=F32)
            dst[:, rows] = jnp.where(low_half, out[:S], out[S:])

    def near(dst, first, count):
        def step(at, _):
            near_pairs(dst, [first + at * 16 + k for k in range(16)])
            return 0

        lax.fori_loop(0, count // 16, step, 0)

    def near_edges(dst):
        near_pairs(dst, list(range(8)) + [leaves // 2 - 8 + j for j in range(8)])

    def columns(app, half):
        arrived(zr.at[app, 0, pl.ds(0, n_col - 1)], zr_sem.at[app, at_half(half)])
        for c in range(4):
            tiles = [zr[app, half, 4 * c + i] for i in range(4)]
            for j, tile in enumerate(blocks_swapped(tiles)):
                zt[slot_of(half, j), c] = tile

    def mix_columns(app, half):
        to_rows = [2 * half + lax.rem(lax.rem(row, 2) + k, 2) + 4 * lax.rem(lax.div(row, 4) + m, 2) for m, k in ((1, 0), (1, 1), (0, 1), (0, 0))]
        for first in (0, 2):
            made = []
            for j in to_rows[first : first + 2]:
                z = jnp.concatenate([zt[j, c] for c in range(4)], axis=1)
                made.append(dot(z, mc[j]).astype(BF16))
            for at, j, t in zip((first, first + 1), to_rows[first:], made):
                stays = half is home and at == 3
                for p in range(4):
                    if stays:
                        tr[app, row, p] = t[:, 128 * p : 128 * (p + 1)]
                    else:
                        ts[app, j, p] = t[:, 128 * p : 128 * (p + 1)]
                if not stays:
                    send(ts.at[app, j], tr.at[app, row], sent.at[2], tr_sem.at[app, at_half(half)], (j, col))

    def rows(app, half):
        arrived(tr.at[app, pl.ds(0, 4 if half is away else 3)], tr_sem.at[app, at_half(half)])
        for p in range(4):
            tiles = [tr[app, slot_of(half, i), p] for i in range(4)]
            for j, tile in enumerate(blocks_swapped(tiles)):
                tt[4 * p + j, half] = tile

    def part_of_rows(p, half):
        weights = [mr[p, pl.ds(pl.multiple_of(64 * half + 128 * i, 64), 64), :] for i in range(2)]
        return dot(tt[p, half], jnp.concatenate(weights, axis=0))

    def mix_rows_first(half):
        for at in range(0, n_col, 8):
            for p in range(at, at + 8):
                tp[p] = part_of_rows(p, half)

    def mix_rows(half):
        for at in range(0, n_col, 8):
            made = [(tp[p] + part_of_rows(p, half)).astype(BF16) for p in range(at, at + 8)]
            for p, t in zip(range(at, at + 8), made):
                one, two = t[:, 0:128], t[:, 128:256]
                t2[0, p] = jnp.where(low_half, one, pltpu.roll(two, 64, 1))
                t2[1, p] = jnp.where(low_half, pltpu.roll(one, 64, 1), two)

    def last_expand(dst):
        zero = jnp.zeros((S, 128), F32)
        rd, bd, dd = zero, zero, zero
        for at in range(0, 2 * n_col, 8):
            fars = [dot(t2[k % 2, k // 2], uq[128 * k : 128 * (k + 1), :]) for k in range(at, at + 8)]
            for k, far in zip(range(at, at + 8), fars):
                for part in range(2):
                    base = 512 * (k // 2) + 128 * (k % 2) + 256 * part
                    lanes = slice(base, base + 128)
                    out = dst[:, lanes] + far[:, 128 * part : 128 * (part + 1)]
                    dst[:, lanes] = out
                    rd, bd, dd = rd + rv[:, lanes] * out, bd + bv[:, lanes] * out, dd + out * out
        return rd, bd, dd

    def placed(packed, qs, sums):
        small = lax.broadcasted_iota(jnp.int32, (8, 128), 1)
        for q, products in zip(qs, sums):
            column = jnp.sum(products, axis=1, keepdims=True)
            for g in range(S // 8):
                packed = jnp.where(small == 8 * g + q, column[8 * g : 8 * (g + 1)], packed)
        return packed

    def early_sums():
        def step(at, carry):
            for k in range(16):
                lanes = pl.ds(pl.multiple_of((at * 16 + k) * 128, 128), 128)
                rx, bx = rv[:, lanes], bv[:, lanes]
                carry = (carry[0] + rx * rx, carry[1] + rx * bx, carry[2] + bx * bx)
            return carry

        zero = jnp.zeros((S, 128), F32)
        return lax.fori_loop(0, leaves // 32, step, (zero, zero, zero))

    def at(name):
        return jax.named_scope(name)

    set_turn()
    met = []

    def meet():
        if not met:
            pl.semaphore_wait(barrier, len(partners))
            met.append(True)

    later = []

    def others():
        for at, (src, dst) in enumerate(((mc_hbm, mc), (u_hbm, uraw), (mr_hbm, mr))):
            later.append(loads(2 + at, src, dst))

    with at("z0"):
        first_compress(meet, others)
        mc_load, u_load, mr_load = later
        send_edges(0, rv)
    with at("spread0"):
        spread(rv)
    with at("expand_w"):
        w_load.wait()
        expand_w(0, leaves // 16)
    mc_load.wait()
    with at("colA0"):
        columns(0, home)
    with at("mixA0"):
        mix_columns(0, home)
    with at("colB0"):
        columns(0, away)
    with at("mixB0"):
        mix_columns(0, away)
    with at("expand_u"):
        u_load.wait()
        expand_u()
    with at("near0"):
        off_load.wait()
        near(bv, 8, inner)
    with at("edges0"):
        spread_edges(0)
        near_edges(bv)
    with at("rowA0"):
        rows(0, home)
        mr_load.wait()
        mix_rows_first(home)
    with at("rowB0"):
        rows(0, away)
    with at("mixrow0"):
        mix_rows(away)
    with at("expz0"):
        expand_and_compress(0, bv)
        send_edges(1, bv)
    with at("spread1"):
        spread(bv)
    with at("sums"):
        packed = placed(jnp.zeros((8, 128), F32), (0, 1, 2), early_sums())
    with at("near1a"):
        near(dv, 8, 16)
    with at("colA1"):
        columns(1, home)
    with at("mixA1"):
        mix_columns(1, home)
    with at("colB1"):
        columns(1, away)
    with at("mixB1"):
        mix_columns(1, away)
    with at("near1b"):
        near(dv, 24, inner - 16)
    with at("edges1"):
        spread_edges(1)
        near_edges(dv)
    with at("rowA1"):
        rows(1, home)
        mix_rows_first(home)
    with at("rowB1"):
        rows(1, away)
    with at("mixrow1"):
        mix_rows(away)
    with at("expand1"):
        rd, bd, dd = last_expand(dv)

    with at("reduce"):
        packed = placed(packed, (3, 4, 5), (rd, bd, dd))
        line = lax.broadcasted_iota(jnp.int32, (8, 128), 0)

        def by_line(shifts, x):
            out = x
            for k in range(1, 4):
                out = jnp.where(lax.rem(line, 4) == k, pltpu.roll(x, shifts[k], 1), out)
            return out

        packed = by_line((0, 32, 64, 96), packed)
        packed = packed + pltpu.roll(packed, 7, 0)
        packed = packed + pltpu.roll(packed, 6, 0)
        mine = jnp.concatenate([packed[0:1], packed[4:5]], axis=0)
        g[...] = mine
        h[flat] = mine
        x_at = lax.div(row, 2)
        far = lambda d: min(d, 4 - d)
        ways = [(dx, dc, k) for dx in range(4) for dc in range(2) for k in range(n_col)]
        ways.sort(key=lambda w: -far(w[0]) - far(steps[w[2]][0]) - far(steps[w[2]][1]) - 0.5 * w[1])
        lines = {(dx, dc): 2 * lax.rem(x_at + dx, 4) + lax.rem(row + dc, 2) for dx in range(4) for dc in range(2)}
        for dx, dc, k in ways[:-1]:
            send(g, h.at[flat], sent.at[3], h_sem, (lines[dx, dc], order[k]))
        with at("red"):
            arrived(h.at[pl.ds(0, total - 1)], h_sem)
        sums = [h[k] for k in range(4)]
        for k in range(4, total):
            sums[k % 4] = sums[k % 4] + h[k]
        both = (sums[0] + sums[1]) + (sums[2] + sums[3])
        packed = by_line((0, 96, 64, 32), jnp.where(line < 4, both[0:1], both[1:2]))

    with at("coefs"):
        rr, rb, bb, rd, bd, dd = (packed if q == 0 else pltpu.roll(packed, 128 - q, 1) for q in range(6))
        inv = 1.0 / rr
        shift = rb * inv
        h21s = bb * inv - shift * shift
        inv_h21s = 1.0 / h21s
        h21 = jnp.sqrt(h21s)
        inv_h21 = h21 * inv_h21s
        h11 = 1.0 + shift
        h12 = (rd - shift * rb) * (inv * inv_h21)
        k22 = (bd - shift * (bb + rd - shift * rb)) * (inv * inv_h21s)
        size = (dd - shift * (2.0 * bd - shift * bb)) * (inv * inv_h21s)
        h32s = size - h12 * h12 - k22 * k22
        h22 = 1.0 + k22
        m11 = h11 * h11 + h21s
        m12 = h11 * h12 + h21 * h22
        m22 = h12 * h12 + h22 * h22 + h32s
        inv_det = 1.0 / (m11 * m22 - m12 * m12)
        y1 = (m22 * h11 - m12 * h12) * inv_det
        y2 = (m11 * h12 - m12 * h11) * inv_det * inv_h21
        for q, x in enumerate((y1 - y2 * shift, y2, 1.0 - y1 + y2 * shift, y1 + y2 - y2 * shift)):
            for g in range(S // 8):
                coefs[q, 8 * g : 8 * (g + 1)] = jnp.broadcast_to(x[:, 8 * g : 8 * g + 1], (8, 128))

    with at("drain"):
        arrived(hs, sent.at[0])
        arrived(zs.at[:, :, pl.ds(0, n_col - 1)], sent.at[1])
        arrived(ts.at[:, pl.ds(0, n_row - 1)], sent.at[2])
        arrived(h.at[pl.ds(0, total - 1)], sent.at[3])


def finish(rv, bv, dv, coefs, sol_hbm, res_hbm, sol, res, sem):
    copies = []
    for g in range(S // 8):
        rows = slice(8 * g, 8 * (g + 1))
        sol_r, sol_b, res_r, res_b = (coefs[q, rows] for q in range(4))
        for at in range(0, rv.shape[1], 128):
            lanes = slice(at, at + 128)
            r, b, d = rv[rows, lanes], bv[rows, lanes], dv[rows, lanes]
            sol[rows, lanes] = sol_r * r + sol_b * b
            res[rows, lanes] = res_r * r - res_b * b - sol_b * d
        for k, (src, dst) in enumerate(((sol, sol_hbm), (res, res_hbm))):
            copies.append(pltpu.make_async_copy(src.at[rows], dst.at[rows], sem.at[k, g]))
            copies[-1].start()
    for copy in copies:
        copy.wait()


def solution(mesh):
    n_row, n_col = mesh.shape["row"], mesh.shape["col"]

    def body(rhs, near_blocks, near_offsets, v_factor, mix_col, mix_row, u_factor):
        leaves = near_offsets.shape[0]
        unknowns = leaves * LEAF
        w = near_blocks.reshape(leaves, 4, 32, 128).transpose(0, 2, 1, 3).reshape(leaves * 128, 128)
        by_tile = lambda x: x.reshape(leaves // 8, 8, 16, 128).transpose(0, 2, 1, 3).reshape(leaves * 16, 128)
        any_spec = pl.BlockSpec(memory_space=pl.ANY)
        field = pltpu.VMEM((S, unknowns), F32)
        vmem_spec = pl.BlockSpec(memory_space=pltpu.VMEM)
        parts = pl.pallas_call(
            functools.partial(kernel, n_row, n_col),
            out_shape=[field, field, field, pltpu.VMEM((4, S, 128), F32)],
            in_specs=[pl.BlockSpec(memory_space=pltpu.HBM)] * 7,
            out_specs=[vmem_spec] * 4,
            scratch_shapes=[
                pltpu.SMEM((4, leaves), jnp.int32),
                pltpu.VMEM((leaves * 128, 128), BF16),
                pltpu.VMEM((leaves * 64, 256), BF16),
                pltpu.VMEM((leaves * 16, 128), BF16),
                pltpu.VMEM((2, n_col, 256, 128), BF16),
                pltpu.VMEM((leaves * 16, 128), BF16),
                pltpu.VMEM((leaves * 32, 256), BF16),
                pltpu.VMEM(mix_col.shape[1:], BF16),
                pltpu.VMEM(mix_row.shape[1:], BF16),
                pltpu.VMEM((leaves + 2 * HALO, S, 128), BF16),
                pltpu.VMEM((256, 256), BF16),
                pltpu.VMEM((2, 2, S, HALO * LEAF), BF16),
                pltpu.VMEM((2, 2, S, HALO * LEAF), BF16),
                pltpu.VMEM((2, 2, n_col, S, 128), BF16),
                pltpu.VMEM((2, 2, n_col, S, 128), BF16),
                pltpu.VMEM((n_row, 4, S, 128), BF16),
                pltpu.VMEM((2, n_row, 4, S, 128), BF16),
                pltpu.VMEM((2, n_row, 4, S, 128), BF16),
                pltpu.VMEM((n_col, 2, S, 128), BF16),
                pltpu.VMEM((n_col, S, n_row * RANK), F32),
                pltpu.VMEM((2, n_col, S, 128), BF16),
                pltpu.VMEM((n_col, 128, 128), F32),
                pltpu.VMEM((16, 128, 128), F32),
                pltpu.VMEM((16, 128, 128), F32),
                pltpu.VMEM((2, 128), F32),
                pltpu.VMEM((n_row * n_col, 2, 128), F32),
                pltpu.SemaphoreType.DMA((5 + 2 * 4,)),
                pltpu.SemaphoreType.DMA((4,)),
                pltpu.SemaphoreType.DMA((2,)),
                pltpu.SemaphoreType.DMA((2, 2)),
                pltpu.SemaphoreType.DMA((2, 2)),
                pltpu.SemaphoreType.DMA,
            ],
            compiler_params=pltpu.CompilerParams(
                collective_id=0, has_side_effects=True, vmem_limit_bytes=54 * 1024 * 1024
            ),
        )(
            rhs, w, near_offsets.T, by_tile(v_factor),
            mix_col[0], mix_row[0], by_tile(u_factor),
        )
        return pl.pallas_call(
            finish,
            out_shape=[jax.ShapeDtypeStruct((S, unknowns), F32)] * 2,
            in_specs=[vmem_spec] * 4,
            out_specs=[any_spec] * 2,
            scratch_shapes=[
                pltpu.VMEM((S, unknowns), F32),
                pltpu.VMEM((S, unknowns), F32),
                pltpu.SemaphoreType.DMA((2, S // 8)),
            ],
            compiler_params=pltpu.CompilerParams(vmem_limit_bytes=8 * 1024 * 1024),
        )(*(pltpu.with_memory_space_constraint(x, pltpu.VMEM) for x in parts))

    both = ("row", "col")
    return jax.shard_map(
        body,
        mesh=mesh,
        in_specs=(
            P(None, both),
            P(both, None, None),
            P(both, None),
            P(both, None),
            P("row", "col", None, None),
            P("row", "col", None, None),
            P(both, None),
        ),
        out_specs=(P(None, both), P(None, both)),
        check_vma=False,
    )
```

```python
import functools

import jax
import jax.numpy as jnp
from jax import lax
from jax.experimental import pallas as pl
from jax.experimental.pallas import tpu as pltpu
from jax.sharding import PartitionSpec as P

S = 32
LEAF = 64
RANK = 32
HALO = 4
F32 = jnp.float32
BF16 = jnp.bfloat16
MESH = pl.DeviceIdType.MESH
NT = (((1,), (1,)), ((), ()))


def dot(a, b):
    return jnp.dot(a, b, preferred_element_type=F32)


def lane_index():
    return lax.broadcasted_iota(jnp.int32, (S, 128), 1)


def blocks_swapped(tiles):
    lane = lane_index()
    low_half = lane < 64
    low_quarter = lax.rem(lane, 64) < 32
    a, b, c, d = tiles
    turn = lambda x, by: pltpu.roll(x, by, 1)
    a, c = jnp.where(low_half, a, turn(c, 64)), jnp.where(low_half, turn(a, 64), c)
    b, d = jnp.where(low_half, b, turn(d, 64)), jnp.where(low_half, turn(b, 64), d)
    a, b = jnp.where(low_quarter, a, turn(b, 32)), jnp.where(low_quarter, turn(a, 96), b)
    c, d = jnp.where(low_quarter, c, turn(d, 32)), jnp.where(low_quarter, turn(c, 96), d)
    return a, b, c, d


def kernel(
    n_row, n_col,
    r_hbm, w_hbm, off_hbm, v_hbm, mc_hbm, mr_hbm, u_hbm,
    rv, bv, dv, coefs,
    off, wraw, wp, vraw, vq, uraw, uq, mc, mr, xd, turn,
    hs, hr, zs, zr, zt, ts, tr, tt, tp, t2, sv, sa, sb, g, h,
    load_sem, sent, hr_sem, zr_sem, tr_sem, h_sem,
):
    row = lax.axis_index("row")
    col = lax.axis_index("col")
    flat = row * n_col + col
    total = n_row * n_col
    leaves = off_hbm.shape[1]
    lane = lane_index()
    low_half = lane < 64

    def loads(index, src, dst):
        copy = pltpu.make_async_copy(src, dst, load_sem.at[index])
        copy.start()
        return copy

    for piece in range(4):
        rows = pl.ds(piece * (leaves * 4), leaves * 4)
        pltpu.make_async_copy(v_hbm.at[rows], vraw.at[rows], load_sem.at[5]).start()
    for piece in range(4):
        rows = pl.ds(piece * (S // 4), S // 4)
        pltpu.make_async_copy(r_hbm.at[rows], rv.at[rows], load_sem.at[6]).start()
    off_load = loads(0, off_hbm, off)
    w_load = loads(1, w_hbm, wraw)

    col_slow, col_fast, row_fast = lax.div(col, 4), lax.rem(col, 4), lax.rem(row, 4)
    home = lax.rem(lax.div(row, 2), 2)
    away = 1 - home

    def slot_of(half, i):
        return 2 * half + (i % 2) + 4 * (i // 2)

    steps = [(z, y) for z in range(4) for y in range(4)]
    steps.sort(key=lambda d: -min(d[0], 4 - d[0]) - min(d[1], 4 - d[1]))
    order = [4 * lax.rem(col_slow + z, 4) + lax.rem(col_fast + y, 4) for z, y in steps]
    own = order[-1]
    inner = leaves // 2 - 16

    def at_half(half):
        return 0 if half is home else 1

    def other_col(k):
        return lax.rem(col + k, n_col)

    def other_row(k):
        return lax.rem(row + k, n_row)

    def at_flat(k):
        other = lax.rem(flat + k, total)
        return (lax.div(other, n_col), lax.rem(other, n_col))

    up, down = at_flat(1), at_flat(total - 1)
    barrier = pltpu.get_barrier_semaphore()
    partners = [(row, other_col(k)) for k in range(1, n_col)]
    partners += [(other_row(k), col) for k in range(1, n_row)] + [up, down]
    for partner in partners:
        pl.semaphore_signal(barrier, inc=1, device_id=partner, device_id_type=MESH)

    def send(src, dst, send_sem, recv_sem, device):
        pltpu.make_async_remote_copy(
            src_ref=src, dst_ref=dst, send_sem=send_sem, recv_sem=recv_sem,
            device_id=device, device_id_type=MESH,
        ).start()

    def arrived(all_of_them, recv_sem):
        pltpu.make_async_copy(all_of_them, all_of_them, recv_sem).wait()

    def set_turn():
        m = lax.broadcasted_iota(jnp.int32, (256, 256), 0)
        n = lax.broadcasted_iota(jnp.int32, (256, 256), 1)
        source = (n // 64) * 64 + 4 * lax.rem(n, 16) + lax.rem(n, 64) // 16
        turn[...] = jnp.where(m == source, 1.0, 0.0).astype(BF16)

    def expand_v(k, half):
        group = lax.broadcasted_iota(jnp.int32, (16, 128), 1) // RANK
        pieces = []
        for j in range(4):
            part = sv[k, pl.ds(slot_of(half, j), 16, stride=8), :].astype(BF16)
            for w in range(4):
                turned = part if j == w else pltpu.roll(part, ((j - w) % 4) * RANK, 1)
                pieces.append(jnp.where(group == j, turned, jnp.zeros_like(turned)))
        vq[at_half(half), k] = jnp.concatenate(pieces, axis=0)

    def expand_u():
        half = lax.broadcasted_iota(jnp.int32, (16, 128), 1) // LEAF
        nothing = jnp.zeros((64, 128), BF16)

        def step(at, _):
            for k in range(8):
                one(8 * at + k, k)
            return 0

        def one(at, k):
            sa[k] = uraw[pl.ds(pl.multiple_of(at * 128, 128), 128), :].astype(F32)
            for leaf in range(8):
                half_at, q = (leaf // 2) % 2, leaf % 2 + 2 * (leaf // 4)
                part = sa[k, pl.ds(leaf, 16, stride=8), :]
                turned = pltpu.roll(part, 64, 1)
                for w in range(2):
                    sb[2 * k + half_at, pl.ds(q * RANK + w, 16, stride=2), :] = jnp.where(
                        half == q % 2, part if w == q % 2 else turned, 0.0
                    )
            for q in range(2):
                base = pl.multiple_of(at * 256 + q * 128, 128)
                uq[pl.ds(base, 64), 0:128] = sb[2 * k + q, 0:64].astype(BF16)
                uq[pl.ds(base, 64), 128:256] = nothing
                uq[pl.ds(base + 64, 64), 0:128] = nothing
                uq[pl.ds(base + 64, 64), 128:256] = sb[2 * k + q, 64:128].astype(BF16)

        lax.fori_loop(0, leaves // 64, step, 0)

    def expand_w(first, last):
        half = lax.broadcasted_iota(jnp.int32, (32, 128), 1) < 64

        def step(at, _):
            for k in range(16):
                leaf = at * 16 + k
                sa[k] = wraw[pl.ds(pl.multiple_of(leaf * 128, 128), 128), :].astype(F32)
            for k in range(16):
                for b in range(2):
                    one = sa[k, pl.ds(2 * b, 32, stride=4), :]
                    two = sa[k, pl.ds(2 * b + 1, 32, stride=4), :]
                    sb[k, pl.ds(64 * b, 32, stride=2), :] = jnp.where(half, one, pltpu.roll(two, 64, 1))
                    sb[k, pl.ds(64 * b + 1, 32, stride=2), :] = jnp.where(half, pltpu.roll(one, 64, 1), two)
            for k in range(16):
                base = pl.multiple_of((at * 16 + k) * 64, 64)
                wp[pl.ds(base, 64), 0:128] = sb[k, 0:64].astype(BF16)
                wp[pl.ds(base, 64), 128:256] = sb[k, 64:128].astype(BF16)
            return 0

        lax.fori_loop(first, last, step, 0)

    def send_edges(app, src):
        hs[app, 0] = src[:, 0 : HALO * LEAF].astype(BF16)
        hs[app, 1] = src[:, (leaves - HALO) * LEAF : leaves * LEAF].astype(BF16)
        send(hs.at[app, 0], hr.at[app, 1], sent.at[0], hr_sem.at[app], down)
        send(hs.at[app, 1], hr.at[app, 0], sent.at[0], hr_sem.at[app], up)

    def field(src, to, half):
        return jnp.concatenate([src[:, lanes] for lanes in tiles_of(to, half)], axis=1)

    def turned_fields(values):
        x = jnp.concatenate([x.astype(BF16) for x in values], axis=0)
        x = dot(x, turn[...]).astype(BF16)
        return [x[S * k : S * (k + 1)] for k in range(len(values))]

    def compress(app, half, ks, fields):
        h = at_half(half)
        made = [dot(x, vq[h, k]).astype(BF16) for k, x in zip(ks, fields)]
        for k, z in zip(ks, made):
            if k == n_col - 1:
                zr[app, half, col] = z
            else:
                zs[app, h, k] = z
        for k in ks:
            if k < n_col - 1:
                send(zs.at[app, h, k], zr.at[app, half, col], sent.at[1], zr_sem.at[app, h], (row, order[k]))

    def tiles_of(to, half):
        return [pl.ds(pl.multiple_of(to * 512 + half * 128 + part * 256, 128), 128) for part in range(2)]

    def first_compress(ready, others):
        ks = list(range(n_col))
        for half in (home, away):
            if half is home:
                pltpu.make_async_copy(v_hbm, vraw, load_sem.at[5]).wait()
                for k in ks:
                    sv[k] = vraw[pl.ds(pl.multiple_of(order[k] * 128, 128), 128), :].astype(F32)
                pltpu.make_async_copy(r_hbm, rv, load_sem.at[6]).wait()
            for k in ks:
                expand_v(k, half)
            fields = turned_fields([field(rv, to, half) for to in order])
            if half is home:
                ready()
            compress(0, half, ks, fields)
            if half is home:
                others()

    def expand_and_compress(app, dst):
        for half in (home, away):
            fields = turned_fields(far_added(dst, half, order))
            compress(app + 1, half, list(range(n_col)), fields)

    def far_added(dst, half, tos):
        fars = [
            dot(t2[half, to], uq[pl.ds(pl.multiple_of((2 * to + half) * 128, 128), 128), :]) for to in tos
        ]
        old = [field(dst, to, half) for to in tos]
        outs = [x + far for x, far in zip(old, fars)]
        for to, out in zip(tos, outs):
            for part, lanes in enumerate(tiles_of(to, half)):
                dst[:, lanes] = out[:, 128 * part : 128 * (part + 1)]
        return outs

    def put_leaves(at, x):
        turned = pltpu.roll(x, 64, 1)
        xd[at] = jnp.where(low_half, x, turned)
        xd[at + 1] = jnp.where(low_half, turned, x)

    def spread(src):
        def step(at, _):
            for k in range(32):
                pair = at * 32 + k
                put_leaves(HALO + 2 * pair, src[:, pl.ds(pl.multiple_of(pair * 128, 128), 128)].astype(BF16))
            return 0

        lax.fori_loop(0, leaves // 64, step, 0)

    def spread_edges(app):
        arrived(hr.at[app], hr_sem.at[app])
        for side, inside in ((0, flat > 0), (1, flat < total - 1)):
            for pair in range(HALO // 2):
                x = hr[app, side, :, pair * 128 : (pair + 1) * 128]
                x = jnp.where(inside, x, jnp.zeros_like(x))
                put_leaves(side * (HALO + leaves) + 2 * pair, x)

    def near_pairs(dst, pairs):
        for pair in pairs:
            parts = []
            for leaf in (2 * pair, 2 * pair + 1):
                index = [leaf + HALO + off[b, leaf] for b in range(4)]
                parts.append(
                    jnp.concatenate(
                        [
                            jnp.where(low_half, xd[index[0]], xd[index[1]]),
                            jnp.where(low_half, xd[index[2]], xd[index[3]]),
                        ],
                        axis=1,
                    )
                )
            lhs = jnp.concatenate(parts, axis=0)
            rows = pl.ds(pair * 128 if isinstance(pair, int) else pl.multiple_of(pair * 128, 128), 128)
            out = lax.dot_general(lhs, wp[rows, :], NT, preferred_element_type=F32)
            dst[:, rows] = jnp.where(low_half, out[:S], out[S:])

    def near(dst, first, count):
        def step(at, _):
            near_pairs(dst, [first + at * 16 + k for k in range(16)])
            return 0

        lax.fori_loop(0, count // 16, step, 0)

    def near_edges(dst):
        near_pairs(dst, list(range(8)) + [leaves // 2 - 8 + j for j in range(8)])

    def columns(app, half):
        arrived(zr.at[app, 0, pl.ds(0, n_col - 1)], zr_sem.at[app, at_half(half)])
        for c in range(4):
            tiles = [zr[app, half, 4 * c + i] for i in range(4)]
            for j, tile in enumerate(blocks_swapped(tiles)):
                zt[slot_of(half, j), c] = tile

    def mix_columns(app, half):
        to_rows = [2 * half + lax.rem(lax.rem(row, 2) + k, 2) + 4 * lax.rem(lax.div(row, 4) + m, 2) for m, k in ((1, 0), (1, 1), (0, 1), (0, 0))]
        made = []
        for j in to_rows:
            z = jnp.concatenate([zt[j, c] for c in range(4)], axis=1)
            made.append(dot(z, mc[j]).astype(BF16))
        for at, (j, t) in enumerate(zip(to_rows, made)):
            stays = half is home and at == 3
            for p in range(4):
                if stays:
                    tr[app, row, p] = t[:, 128 * p : 128 * (p + 1)]
                else:
                    ts[app, j, p] = t[:, 128 * p : 128 * (p + 1)]
            if not stays:
                send(ts.at[app, j], tr.at[app, row], sent.at[2], tr_sem.at[app, at_half(half)], (j, col))

    def rows(app, half):
        arrived(tr.at[app, pl.ds(0, 4 if half is away else 3)], tr_sem.at[app, at_half(half)])
        for p in range(4):
            tiles = [tr[app, slot_of(half, i), p] for i in range(4)]
            for j, tile in enumerate(blocks_swapped(tiles)):
                tt[4 * p + j, half] = tile

    def part_of_rows(p, half):
        weights = [mr[p, pl.ds(pl.multiple_of(64 * half + 128 * i, 64), 64), :] for i in range(2)]
        return dot(tt[p, half], jnp.concatenate(weights, axis=0))

    def mix_rows_first(half):
        for at in range(0, n_col, 8):
            for p in range(at, at + 8):
                tp[p] = part_of_rows(p, half)

    def mix_rows(half):
        for at in range(0, n_col, 8):
            made = [(tp[p] + part_of_rows(p, half)).astype(BF16) for p in range(at, at + 8)]
            for p, t in zip(range(at, at + 8), made):
                one, two = t[:, 0:128], t[:, 128:256]
                t2[0, p] = jnp.where(low_half, one, pltpu.roll(two, 64, 1))
                t2[1, p] = jnp.where(low_half, pltpu.roll(one, 64, 1), two)

    def last_expand(dst):
        zero = jnp.zeros((S, 128), F32)
        rd, bd, dd = zero, zero, zero
        for at in range(0, 2 * n_col, 8):
            fars = [dot(t2[k % 2, k // 2], uq[128 * k : 128 * (k + 1), :]) for k in range(at, at + 8)]
            for k, far in zip(range(at, at + 8), fars):
                for part in range(2):
                    base = 512 * (k // 2) + 128 * (k % 2) + 256 * part
                    lanes = slice(base, base + 128)
                    out = dst[:, lanes] + far[:, 128 * part : 128 * (part + 1)]
                    dst[:, lanes] = out
                    rd, bd, dd = rd + rv[:, lanes] * out, bd + bv[:, lanes] * out, dd + out * out
        return rd, bd, dd

    def placed(packed, qs, sums):
        small = lax.broadcasted_iota(jnp.int32, (8, 128), 1)
        for q, products in zip(qs, sums):
            column = jnp.sum(products, axis=1, keepdims=True)
            for g in range(S // 8):
                packed = jnp.where(small == 8 * g + q, column[8 * g : 8 * (g + 1)], packed)
        return packed

    def early_sums():
        def step(at, carry):
            for k in range(16):
                lanes = pl.ds(pl.multiple_of((at * 16 + k) * 128, 128), 128)
                rx, bx = rv[:, lanes], bv[:, lanes]
                carry = (carry[0] + rx * rx, carry[1] + rx * bx, carry[2] + bx * bx)
            return carry

        zero = jnp.zeros((S, 128), F32)
        return lax.fori_loop(0, leaves // 32, step, (zero, zero, zero))

    def at(name):
        return jax.named_scope(name)

    set_turn()
    met = []

    def meet():
        if not met:
            pl.semaphore_wait(barrier, len(partners))
            met.append(True)

    later = []

    def others():
        for at, (src, dst) in enumerate(((mc_hbm, mc), (u_hbm, uraw), (mr_hbm, mr))):
            later.append(loads(2 + at, src, dst))

    with at("z0"):
        first_compress(meet, others)
        mc_load, u_load, mr_load = later
        send_edges(0, rv)
    with at("spread0"):
        spread(rv)
    with at("expand_w"):
        w_load.wait()
        expand_w(0, leaves // 16)
    mc_load.wait()
    with at("colA0"):
        columns(0, home)
    with at("mixA0"):
        mix_columns(0, home)
    with at("colB0"):
        columns(0, away)
    with at("mixB0"):
        mix_columns(0, away)
    with at("expand_u"):
        u_load.wait()
        expand_u()
    with at("near0"):
        off_load.wait()
        near(bv, 8, inner)
    with at("edges0"):
        spread_edges(0)
        near_edges(bv)
    with at("rowA0"):
        rows(0, home)
        mr_load.wait()
        mix_rows_first(home)
    with at("rowB0"):
        rows(0, away)
    with at("mixrow0"):
        mix_rows(away)
    with at("expz0"):
        expand_and_compress(0, bv)
        send_edges(1, bv)
    with at("spread1"):
        spread(bv)
    with at("sums"):
        packed = placed(jnp.zeros((8, 128), F32), (0, 1, 2), early_sums())
    with at("near1a"):
        near(dv, 8, 16)
    with at("colA1"):
        columns(1, home)
    with at("mixA1"):
        mix_columns(1, home)
    with at("colB1"):
        columns(1, away)
    with at("mixB1"):
        mix_columns(1, away)
    with at("near1b"):
        near(dv, 24, inner - 16)
    with at("edges1"):
        spread_edges(1)
        near_edges(dv)
    with at("rowA1"):
        rows(1, home)
        mix_rows_first(home)
    with at("rowB1"):
        rows(1, away)
    with at("mixrow1"):
        mix_rows(away)
    with at("expand1"):
        rd, bd, dd = last_expand(dv)

    with at("reduce"):
        packed = placed(packed, (3, 4, 5), (rd, bd, dd))
        line = lax.broadcasted_iota(jnp.int32, (8, 128), 0)

        def by_line(shifts, x):
            out = x
            for k in range(1, 4):
                out = jnp.where(lax.rem(line, 4) == k, pltpu.roll(x, shifts[k], 1), out)
            return out

        packed = by_line((0, 32, 64, 96), packed)
        packed = packed + pltpu.roll(packed, 7, 0)
        packed = packed + pltpu.roll(packed, 6, 0)
        mine = jnp.concatenate([packed[0:1], packed[4:5]], axis=0)
        g[...] = mine
        h[flat] = mine
        x_at = lax.div(row, 2)
        far = lambda d: min(d, 4 - d)
        ways = [(dx, dc, k) for dx in range(4) for dc in range(2) for k in range(n_col)]
        ways.sort(key=lambda w: -far(w[0]) - far(steps[w[2]][0]) - far(steps[w[2]][1]) - 0.5 * w[1])
        lines = {(dx, dc): 2 * lax.rem(x_at + dx, 4) + lax.rem(row + dc, 2) for dx in range(4) for dc in range(2)}
        for dx, dc, k in ways[:-1]:
            send(g, h.at[flat], sent.at[3], h_sem, (lines[dx, dc], order[k]))
        with at("red"):
            arrived(h.at[pl.ds(0, total - 1)], h_sem)
        sums = [h[k] for k in range(4)]
        for k in range(4, total):
            sums[k % 4] = sums[k % 4] + h[k]
        both = (sums[0] + sums[1]) + (sums[2] + sums[3])
        packed = by_line((0, 96, 64, 32), jnp.where(line < 4, both[0:1], both[1:2]))

    with at("coefs"):
        rr, rb, bb, rd, bd, dd = (packed if q == 0 else pltpu.roll(packed, 128 - q, 1) for q in range(6))
        inv = 1.0 / rr
        shift = rb * inv
        h21s = bb * inv - shift * shift
        inv_h21s = 1.0 / h21s
        h21 = jnp.sqrt(h21s)
        inv_h21 = h21 * inv_h21s
        h11 = 1.0 + shift
        h12 = (rd - shift * rb) * (inv * inv_h21)
        k22 = (bd - shift * (bb + rd - shift * rb)) * (inv * inv_h21s)
        size = (dd - shift * (2.0 * bd - shift * bb)) * (inv * inv_h21s)
        h32s = size - h12 * h12 - k22 * k22
        h22 = 1.0 + k22
        m11 = h11 * h11 + h21s
        m12 = h11 * h12 + h21 * h22
        m22 = h12 * h12 + h22 * h22 + h32s
        inv_det = 1.0 / (m11 * m22 - m12 * m12)
        y1 = (m22 * h11 - m12 * h12) * inv_det
        y2 = (m11 * h12 - m12 * h11) * inv_det * inv_h21
        for q, x in enumerate((y1 - y2 * shift, y2, 1.0 - y1 + y2 * shift, y1 + y2 - y2 * shift)):
            for g in range(S // 8):
                coefs[q, 8 * g : 8 * (g + 1)] = jnp.broadcast_to(x[:, 8 * g : 8 * g + 1], (8, 128))

    with at("drain"):
        arrived(hs, sent.at[0])
        arrived(zs.at[:, :, pl.ds(0, n_col - 1)], sent.at[1])
        arrived(ts.at[:, pl.ds(0, n_row - 1)], sent.at[2])
        arrived(h.at[pl.ds(0, total - 1)], sent.at[3])


def finish(rv, bv, dv, coefs, sol_hbm, res_hbm, sol, res, sem):
    width = rv.shape[1] // 2
    for g in range(S // 8):
        rows = slice(8 * g, 8 * (g + 1))
        sol_r, sol_b, res_r, res_b = (coefs[q, rows] for q in range(4))
        for part in range(2):
            for at in range(part * width, (part + 1) * width, 128):
                lanes = slice(at, at + 128)
                r, b, d = rv[rows, lanes], bv[rows, lanes], dv[rows, lanes]
                sol[rows, lanes] = sol_r * r + sol_b * b
                res[rows, lanes] = res_r * r - res_b * b - sol_b * d
            lanes = pl.ds(part * width, width)
            for k, (src, dst) in enumerate(((sol, sol_hbm), (res, res_hbm))):
                pltpu.make_async_copy(src.at[rows, lanes], dst.at[rows, lanes], sem.at[k]).start()
    for k, (src, dst) in enumerate(((sol, sol_hbm), (res, res_hbm))):
        pltpu.make_async_copy(src, dst, sem.at[k]).wait()


def solution(mesh):
    n_row, n_col = mesh.shape["row"], mesh.shape["col"]

    def body(rhs, near_blocks, near_offsets, v_factor, mix_col, mix_row, u_factor):
        leaves = near_offsets.shape[0]
        unknowns = leaves * LEAF
        w = near_blocks.reshape(leaves, 4, 32, 128).transpose(0, 2, 1, 3).reshape(leaves * 128, 128)
        by_tile = lambda x: x.reshape(leaves // 8, 8, 16, 128).transpose(0, 2, 1, 3).reshape(leaves * 16, 128)
        any_spec = pl.BlockSpec(memory_space=pl.ANY)
        field = pltpu.VMEM((S, unknowns), F32)
        vmem_spec = pl.BlockSpec(memory_space=pltpu.VMEM)
        parts = pl.pallas_call(
            functools.partial(kernel, n_row, n_col),
            out_shape=[field, field, field, pltpu.VMEM((4, S, 128), F32)],
            in_specs=[pl.BlockSpec(memory_space=pltpu.HBM)] * 7,
            out_specs=[vmem_spec] * 4,
            scratch_shapes=[
                pltpu.SMEM((4, leaves), jnp.int32),
                pltpu.VMEM((leaves * 128, 128), BF16),
                pltpu.VMEM((leaves * 64, 256), BF16),
                pltpu.VMEM((leaves * 16, 128), BF16),
                pltpu.VMEM((2, n_col, 256, 128), BF16),
                pltpu.VMEM((leaves * 16, 128), BF16),
                pltpu.VMEM((leaves * 32, 256), BF16),
                pltpu.VMEM(mix_col.shape[1:], BF16),
                pltpu.VMEM(mix_row.shape[1:], BF16),
                pltpu.VMEM((leaves + 2 * HALO, S, 128), BF16),
                pltpu.VMEM((256, 256), BF16),
                pltpu.VMEM((2, 2, S, HALO * LEAF), BF16),
                pltpu.VMEM((2, 2, S, HALO * LEAF), BF16),
                pltpu.VMEM((2, 2, n_col, S, 128), BF16),
                pltpu.VMEM((2, 2, n_col, S, 128), BF16),
                pltpu.VMEM((n_row, 4, S, 128), BF16),
                pltpu.VMEM((2, n_row, 4, S, 128), BF16),
                pltpu.VMEM((2, n_row, 4, S, 128), BF16),
                pltpu.VMEM((n_col, 2, S, 128), BF16),
                pltpu.VMEM((n_col, S, n_row * RANK), F32),
                pltpu.VMEM((2, n_col, S, 128), BF16),
                pltpu.VMEM((n_col, 128, 128), F32),
                pltpu.VMEM((16, 128, 128), F32),
                pltpu.VMEM((16, 128, 128), F32),
                pltpu.VMEM((2, 128), F32),
                pltpu.VMEM((n_row * n_col, 2, 128), F32),
                pltpu.SemaphoreType.DMA((7,)),
                pltpu.SemaphoreType.DMA((4,)),
                pltpu.SemaphoreType.DMA((2,)),
                pltpu.SemaphoreType.DMA((2, 2)),
                pltpu.SemaphoreType.DMA((2, 2)),
                pltpu.SemaphoreType.DMA,
            ],
            compiler_params=pltpu.CompilerParams(
                collective_id=0, has_side_effects=True, vmem_limit_bytes=54 * 1024 * 1024
            ),
        )(
            rhs, w, near_offsets.T, by_tile(v_factor),
            mix_col[0], mix_row[0], by_tile(u_factor),
        )
        return pl.pallas_call(
            finish,
            out_shape=[jax.ShapeDtypeStruct((S, unknowns), F32)] * 2,
            in_specs=[vmem_spec] * 4,
            out_specs=[any_spec] * 2,
            scratch_shapes=[
                pltpu.VMEM((S, unknowns), F32),
                pltpu.VMEM((S, unknowns), F32),
                pltpu.SemaphoreType.DMA((2,)),
            ],
            compiler_params=pltpu.CompilerParams(vmem_limit_bytes=8 * 1024 * 1024),
        )(*(pltpu.with_memory_space_constraint(x, pltpu.VMEM) for x in parts))

    both = ("row", "col")
    return jax.shard_map(
        body,
        mesh=mesh,
        in_specs=(
            P(None, both),
            P(both, None, None),
            P(both, None),
            P(both, None),
            P("row", "col", None, None),
            P("row", "col", None, None),
            P(both, None),
        ),
        out_specs=(P(None, both), P(None, both)),
        check_vma=False,
    )
```

```python
import functools

import jax
import jax.numpy as jnp
from jax import lax
from jax.experimental import pallas as pl
from jax.experimental.pallas import tpu as pltpu
from jax.sharding import PartitionSpec as P

S = 32
LEAF = 64
RANK = 32
HALO = 4
F32 = jnp.float32
BF16 = jnp.bfloat16
MESH = pl.DeviceIdType.MESH
NT = (((1,), (1,)), ((), ()))


def dot(a, b):
    return jnp.dot(a, b, preferred_element_type=F32)


def lane_index():
    return lax.broadcasted_iota(jnp.int32, (S, 128), 1)


def blocks_swapped(tiles):
    lane = lane_index()
    low_half = lane < 64
    low_quarter = lax.rem(lane, 64) < 32
    a, b, c, d = tiles
    turn = lambda x, by: pltpu.roll(x, by, 1)
    a, c = jnp.where(low_half, a, turn(c, 64)), jnp.where(low_half, turn(a, 64), c)
    b, d = jnp.where(low_half, b, turn(d, 64)), jnp.where(low_half, turn(b, 64), d)
    a, b = jnp.where(low_quarter, a, turn(b, 32)), jnp.where(low_quarter, turn(a, 96), b)
    c, d = jnp.where(low_quarter, c, turn(d, 32)), jnp.where(low_quarter, turn(c, 96), d)
    return a, b, c, d


def kernel(
    n_row, n_col,
    r_hbm, w_hbm, off_hbm, v_hbm, mc_hbm, mr_hbm, u_hbm,
    rv, bv, dv, coefs,
    off, wraw, wp, vraw, vq, uraw, uq, mc, mr, xd, turn,
    hs, hr, zs, zr, zt, ts, tr, tt, tp, t2, sv, sa, sb, g, h,
    load_sem, sent, hr_sem, zr_sem, tr_sem, h_sem,
):
    row = lax.axis_index("row")
    col = lax.axis_index("col")
    flat = row * n_col + col
    total = n_row * n_col
    leaves = off_hbm.shape[1]
    lane = lane_index()
    low_half = lane < 64

    def loads(index, src, dst):
        copy = pltpu.make_async_copy(src, dst, load_sem.at[index])
        copy.start()
        return copy

    for piece in range(4):
        rows = pl.ds(piece * (leaves * 4), leaves * 4)
        pltpu.make_async_copy(v_hbm.at[rows], vraw.at[rows], load_sem.at[5]).start()
    for piece in range(4):
        rows = pl.ds(piece * (S // 4), S // 4)
        pltpu.make_async_copy(r_hbm.at[rows], rv.at[rows], load_sem.at[6]).start()
    off_load = loads(0, off_hbm, off)
    w_load = loads(1, w_hbm, wraw)

    col_slow, col_fast, row_fast = lax.div(col, 4), lax.rem(col, 4), lax.rem(row, 4)
    home = lax.rem(lax.div(row, 2), 2)
    away = 1 - home

    def slot_of(half, i):
        return 2 * half + (i % 2) + 4 * (i // 2)

    steps = [(z, y) for z in range(4) for y in range(4)]
    steps.sort(key=lambda d: -min(d[0], 4 - d[0]) - min(d[1], 4 - d[1]))
    order = [4 * lax.rem(col_slow + z, 4) + lax.rem(col_fast + y, 4) for z, y in steps]
    own = order[-1]
    inner = leaves // 2 - 16

    def at_half(half):
        return 0 if half is home else 1

    def other_col(k):
        return lax.rem(col + k, n_col)

    def other_row(k):
        return lax.rem(row + k, n_row)

    def at_flat(k):
        other = lax.rem(flat + k, total)
        return (lax.div(other, n_col), lax.rem(other, n_col))

    up, down = at_flat(1), at_flat(total - 1)
    barrier = pltpu.get_barrier_semaphore()
    partners = [(row, other_col(k)) for k in range(1, n_col)]
    partners += [(other_row(k), col) for k in range(1, n_row)] + [up, down]
    for partner in partners:
        pl.semaphore_signal(barrier, inc=1, device_id=partner, device_id_type=MESH)

    def send(src, dst, send_sem, recv_sem, device):
        pltpu.make_async_remote_copy(
            src_ref=src, dst_ref=dst, send_sem=send_sem, recv_sem=recv_sem,
            device_id=device, device_id_type=MESH,
        ).start()

    def arrived(all_of_them, recv_sem):
        pltpu.make_async_copy(all_of_them, all_of_them, recv_sem).wait()

    def set_turn():
        m = lax.broadcasted_iota(jnp.int32, (256, 256), 0)
        n = lax.broadcasted_iota(jnp.int32, (256, 256), 1)
        source = (n // 64) * 64 + 4 * lax.rem(n, 16) + lax.rem(n, 64) // 16
        turn[...] = jnp.where(m == source, 1.0, 0.0).astype(BF16)

    def expand_v(k, half):
        group = lax.broadcasted_iota(jnp.int32, (16, 128), 1) // RANK
        pieces = []
        for j in range(4):
            part = sv[k, pl.ds(slot_of(half, j), 16, stride=8), :].astype(BF16)
            for w in range(4):
                turned = part if j == w else pltpu.roll(part, ((j - w) % 4) * RANK, 1)
                pieces.append(jnp.where(group == j, turned, jnp.zeros_like(turned)))
        vq[at_half(half), k] = jnp.concatenate(pieces, axis=0)

    def expand_u():
        half = lax.broadcasted_iota(jnp.int32, (16, 128), 1) // LEAF
        nothing = jnp.zeros((64, 128), BF16)

        def step(at, _):
            for k in range(8):
                one(8 * at + k, k)
            return 0

        def one(at, k):
            sa[k] = uraw[pl.ds(pl.multiple_of(at * 128, 128), 128), :].astype(F32)
            for leaf in range(8):
                half_at, q = (leaf // 2) % 2, leaf % 2 + 2 * (leaf // 4)
                part = sa[k, pl.ds(leaf, 16, stride=8), :]
                turned = pltpu.roll(part, 64, 1)
                for w in range(2):
                    sb[2 * k + half_at, pl.ds(q * RANK + w, 16, stride=2), :] = jnp.where(
                        half == q % 2, part if w == q % 2 else turned, 0.0
                    )
            for q in range(2):
                base = pl.multiple_of(at * 256 + q * 128, 128)
                uq[pl.ds(base, 64), 0:128] = sb[2 * k + q, 0:64].astype(BF16)
                uq[pl.ds(base, 64), 128:256] = nothing
                uq[pl.ds(base + 64, 64), 0:128] = nothing
                uq[pl.ds(base + 64, 64), 128:256] = sb[2 * k + q, 64:128].astype(BF16)

        lax.fori_loop(0, leaves // 64, step, 0)

    def expand_w(first, last):
        half = lax.broadcasted_iota(jnp.int32, (32, 128), 1) < 64

        def step(at, _):
            for k in range(16):
                leaf = at * 16 + k
                sa[k] = wraw[pl.ds(pl.multiple_of(leaf * 128, 128), 128), :].astype(F32)
            for k in range(16):
                for b in range(2):
                    one = sa[k, pl.ds(2 * b, 32, stride=4), :]
                    two = sa[k, pl.ds(2 * b + 1, 32, stride=4), :]
                    sb[k, pl.ds(64 * b, 32, stride=2), :] = jnp.where(half, one, pltpu.roll(two, 64, 1))
                    sb[k, pl.ds(64 * b + 1, 32, stride=2), :] = jnp.where(half, pltpu.roll(one, 64, 1), two)
            for k in range(16):
                base = pl.multiple_of((at * 16 + k) * 64, 64)
                wp[pl.ds(base, 64), 0:128] = sb[k, 0:64].astype(BF16)
                wp[pl.ds(base, 64), 128:256] = sb[k, 64:128].astype(BF16)
            return 0

        lax.fori_loop(first, last, step, 0)

    def send_edges(app, src):
        hs[app, 0] = src[:, 0 : HALO * LEAF].astype(BF16)
        hs[app, 1] = src[:, (leaves - HALO) * LEAF : leaves * LEAF].astype(BF16)
        send(hs.at[app, 0], hr.at[app, 1], sent, hr_sem.at[app], down)
        send(hs.at[app, 1], hr.at[app, 0], sent, hr_sem.at[app], up)

    def field(src, to, half):
        return jnp.concatenate([src[:, lanes] for lanes in tiles_of(to, half)], axis=1)

    def turned_fields(values):
        x = jnp.concatenate([x.astype(BF16) for x in values], axis=0)
        x = dot(x, turn[...]).astype(BF16)
        return [x[S * k : S * (k + 1)] for k in range(len(values))]

    def compress(app, half, ks, fields):
        h = at_half(half)
        made = [dot(x, vq[h, k]).astype(BF16) for k, x in zip(ks, fields)]
        for k, z in zip(ks, made):
            if k == n_col - 1:
                zr[app, half, col] = z
            else:
                zs[app, h, k] = z
        for k in ks:
            if k < n_col - 1:
                send(zs.at[app, h, k], zr.at[app, half, col], sent, zr_sem.at[app, h], (row, order[k]))

    def tiles_of(to, half):
        return [pl.ds(pl.multiple_of(to * 512 + half * 128 + part * 256, 128), 128) for part in range(2)]

    def first_compress(ready, others):
        ks = list(range(n_col))
        for half in (home, away):
            if half is home:
                pltpu.make_async_copy(v_hbm, vraw, load_sem.at[5]).wait()
                for k in ks:
                    sv[k] = vraw[pl.ds(pl.multiple_of(order[k] * 128, 128), 128), :].astype(F32)
                pltpu.make_async_copy(r_hbm, rv, load_sem.at[6]).wait()
            for k in ks:
                expand_v(k, half)
            fields = turned_fields([field(rv, to, half) for to in order])
            if half is home:
                ready()
            compress(0, half, ks, fields)
            if half is home:
                others()

    def expand_and_compress(app, dst):
        for half in (home, away):
            fields = turned_fields(far_added(dst, half, order))
            compress(app + 1, half, list(range(n_col)), fields)

    def far_added(dst, half, tos):
        fars = [
            dot(t2[half, to], uq[pl.ds(pl.multiple_of((2 * to + half) * 128, 128), 128), :]) for to in tos
        ]
        old = [field(dst, to, half) for to in tos]
        outs = [x + far for x, far in zip(old, fars)]
        for to, out in zip(tos, outs):
            for part, lanes in enumerate(tiles_of(to, half)):
                dst[:, lanes] = out[:, 128 * part : 128 * (part + 1)]
        return outs

    def put_leaves(at, x):
        turned = pltpu.roll(x, 64, 1)
        xd[at] = jnp.where(low_half, x, turned)
        xd[at + 1] = jnp.where(low_half, turned, x)

    def spread(src):
        def step(at, _):
            for k in range(32):
                pair = at * 32 + k
                put_leaves(HALO + 2 * pair, src[:, pl.ds(pl.multiple_of(pair * 128, 128), 128)].astype(BF16))
            return 0

        lax.fori_loop(0, leaves // 64, step, 0)

    def spread_edges(app):
        arrived(hr.at[app], hr_sem.at[app])
        for side, inside in ((0, flat > 0), (1, flat < total - 1)):
            for pair in range(HALO // 2):
                x = hr[app, side, :, pair * 128 : (pair + 1) * 128]
                x = jnp.where(inside, x, jnp.zeros_like(x))
                put_leaves(side * (HALO + leaves) + 2 * pair, x)

    def near_pairs(dst, pairs):
        for pair in pairs:
            parts = []
            for leaf in (2 * pair, 2 * pair + 1):
                index = [leaf + HALO + off[b, leaf] for b in range(4)]
                parts.append(
                    jnp.concatenate(
                        [
                            jnp.where(low_half, xd[index[0]], xd[index[1]]),
                            jnp.where(low_half, xd[index[2]], xd[index[3]]),
                        ],
                        axis=1,
                    )
                )
            lhs = jnp.concatenate(parts, axis=0)
            rows = pl.ds(pair * 128 if isinstance(pair, int) else pl.multiple_of(pair * 128, 128), 128)
            out = lax.dot_general(lhs, wp[rows, :], NT, preferred_element_type=F32)
            dst[:, rows] = jnp.where(low_half, out[:S], out[S:])

    def near(dst, first, count):
        def step(at, _):
            near_pairs(dst, [first + at * 16 + k for k in range(16)])
            return 0

        lax.fori_loop(0, count // 16, step, 0)

    def near_edges(dst):
        near_pairs(dst, list(range(8)) + [leaves // 2 - 8 + j for j in range(8)])

    def columns(app, half):
        arrived(zr.at[app, 0, pl.ds(0, n_col - 1)], zr_sem.at[app, at_half(half)])
        for c in range(4):
            tiles = [zr[app, half, 4 * c + i] for i in range(4)]
            for j, tile in enumerate(blocks_swapped(tiles)):
                zt[slot_of(half, j), c] = tile

    def mix_columns(app, half):
        to_rows = [2 * half + lax.rem(lax.rem(row, 2) + k, 2) + 4 * lax.rem(lax.div(row, 4) + m, 2) for m, k in ((1, 0), (1, 1), (0, 1), (0, 0))]
        made = []
        for j in to_rows:
            z = jnp.concatenate([zt[j, c] for c in range(4)], axis=1)
            made.append(dot(z, mc[j]).astype(BF16))
        for at, (j, t) in enumerate(zip(to_rows, made)):
            stays = half is home and at == 3
            for p in range(4):
                if stays:
                    tr[app, row, p] = t[:, 128 * p : 128 * (p + 1)]
                else:
                    ts[app, j, p] = t[:, 128 * p : 128 * (p + 1)]
            if not stays:
                send(ts.at[app, j], tr.at[app, row], sent, tr_sem.at[app, at_half(half)], (j, col))

    def rows(app, half):
        arrived(tr.at[app, pl.ds(0, 4 if half is away else 3)], tr_sem.at[app, at_half(half)])
        for p in range(4):
            tiles = [tr[app, slot_of(half, i), p] for i in range(4)]
            for j, tile in enumerate(blocks_swapped(tiles)):
                tt[4 * p + j, half] = tile

    def part_of_rows(p, half):
        weights = [mr[p, pl.ds(pl.multiple_of(64 * half + 128 * i, 64), 64), :] for i in range(2)]
        return dot(tt[p, half], jnp.concatenate(weights, axis=0))

    def mix_rows_first(half):
        for at in range(0, n_col, 8):
            for p in range(at, at + 8):
                tp[p] = part_of_rows(p, half)

    def mix_rows(half):
        for at in range(0, n_col, 8):
            made = [(tp[p] + part_of_rows(p, half)).astype(BF16) for p in range(at, at + 8)]
            for p, t in zip(range(at, at + 8), made):
                one, two = t[:, 0:128], t[:, 128:256]
                t2[0, p] = jnp.where(low_half, one, pltpu.roll(two, 64, 1))
                t2[1, p] = jnp.where(low_half, pltpu.roll(one, 64, 1), two)

    def last_expand(dst):
        zero = jnp.zeros((S, 128), F32)
        rd, bd, dd = zero, zero, zero
        for at in range(0, 2 * n_col, 8):
            fars = [dot(t2[k % 2, k // 2], uq[128 * k : 128 * (k + 1), :]) for k in range(at, at + 8)]
            for k, far in zip(range(at, at + 8), fars):
                for part in range(2):
                    base = 512 * (k // 2) + 128 * (k % 2) + 256 * part
                    lanes = slice(base, base + 128)
                    out = dst[:, lanes] + far[:, 128 * part : 128 * (part + 1)]
                    dst[:, lanes] = out
                    rd, bd, dd = rd + rv[:, lanes] * out, bd + bv[:, lanes] * out, dd + out * out
        return rd, bd, dd

    def placed(packed, qs, sums):
        small = lax.broadcasted_iota(jnp.int32, (8, 128), 1)
        for q, products in zip(qs, sums):
            column = jnp.sum(products, axis=1, keepdims=True)
            for g in range(S // 8):
                packed = jnp.where(small == 8 * g + q, column[8 * g : 8 * (g + 1)], packed)
        return packed

    def early_sums():
        def step(at, carry):
            for k in range(16):
                lanes = pl.ds(pl.multiple_of((at * 16 + k) * 128, 128), 128)
                rx, bx = rv[:, lanes], bv[:, lanes]
                carry = (carry[0] + rx * rx, carry[1] + rx * bx, carry[2] + bx * bx)
            return carry

        zero = jnp.zeros((S, 128), F32)
        return lax.fori_loop(0, leaves // 32, step, (zero, zero, zero))

    def at(name):
        return jax.named_scope(name)

    set_turn()
    met = []

    def meet():
        if not met:
            pl.semaphore_wait(barrier, len(partners))
            met.append(True)

    later = []

    def others():
        for at, (src, dst) in enumerate(((mc_hbm, mc), (u_hbm, uraw), (mr_hbm, mr))):
            later.append(loads(2 + at, src, dst))

    with at("z0"):
        first_compress(meet, others)
        mc_load, u_load, mr_load = later
        send_edges(0, rv)
    with at("spread0"):
        spread(rv)
    with at("expand_w"):
        w_load.wait()
        expand_w(0, leaves // 16)
    mc_load.wait()
    with at("colA0"):
        columns(0, home)
    with at("mixA0"):
        mix_columns(0, home)
    with at("colB0"):
        columns(0, away)
    with at("mixB0"):
        mix_columns(0, away)
    with at("expand_u"):
        u_load.wait()
        expand_u()
    with at("near0"):
        off_load.wait()
        near(bv, 8, inner)
    with at("edges0"):
        spread_edges(0)
        near_edges(bv)
    with at("rowA0"):
        rows(0, home)
        mr_load.wait()
        mix_rows_first(home)
    with at("rowB0"):
        rows(0, away)
    with at("mixrow0"):
        mix_rows(away)
    with at("expz0"):
        expand_and_compress(0, bv)
        send_edges(1, bv)
    with at("spread1"):
        spread(bv)
    with at("sums"):
        packed = placed(jnp.zeros((8, 128), F32), (0, 1, 2), early_sums())
    with at("near1a"):
        near(dv, 8, 16)
    with at("colA1"):
        columns(1, home)
    with at("mixA1"):
        mix_columns(1, home)
    with at("colB1"):
        columns(1, away)
    with at("mixB1"):
        mix_columns(1, away)
    with at("near1b"):
        near(dv, 24, inner - 16)
    with at("edges1"):
        spread_edges(1)
        near_edges(dv)
    with at("rowA1"):
        rows(1, home)
        mix_rows_first(home)
    with at("rowB1"):
        rows(1, away)
    with at("mixrow1"):
        mix_rows(away)
    with at("expand1"):
        rd, bd, dd = last_expand(dv)

    with at("reduce"):
        packed = placed(packed, (3, 4, 5), (rd, bd, dd))
        line = lax.broadcasted_iota(jnp.int32, (8, 128), 0)

        def by_line(shifts, x):
            out = x
            for k in range(1, 4):
                out = jnp.where(lax.rem(line, 4) == k, pltpu.roll(x, shifts[k], 1), out)
            return out

        packed = by_line((0, 32, 64, 96), packed)
        packed = packed + pltpu.roll(packed, 7, 0)
        packed = packed + pltpu.roll(packed, 6, 0)
        mine = jnp.concatenate([packed[0:1], packed[4:5]], axis=0)
        g[...] = mine
        h[flat] = mine
        x_at = lax.div(row, 2)
        far = lambda d: min(d, 4 - d)
        ways = [(dx, dc, k) for dx in range(4) for dc in range(2) for k in range(n_col)]
        ways.sort(key=lambda w: -far(w[0]) - far(steps[w[2]][0]) - far(steps[w[2]][1]) - 0.5 * w[1])
        lines = {(dx, dc): 2 * lax.rem(x_at + dx, 4) + lax.rem(row + dc, 2) for dx in range(4) for dc in range(2)}
        for dx, dc, k in ways[:-1]:
            send(g, h.at[flat], sent, h_sem, (lines[dx, dc], order[k]))
        with at("red"):
            arrived(h.at[pl.ds(0, total - 1)], h_sem)
        sums = [h[k] for k in range(4)]
        for k in range(4, total):
            sums[k % 4] = sums[k % 4] + h[k]
        both = (sums[0] + sums[1]) + (sums[2] + sums[3])
        packed = by_line((0, 96, 64, 32), jnp.where(line < 4, both[0:1], both[1:2]))

    with at("coefs"):
        rr, rb, bb, rd, bd, dd = (packed if q == 0 else pltpu.roll(packed, 128 - q, 1) for q in range(6))
        inv = 1.0 / rr
        shift = rb * inv
        h21s = bb * inv - shift * shift
        inv_h21s = 1.0 / h21s
        h21 = jnp.sqrt(h21s)
        inv_h21 = h21 * inv_h21s
        h11 = 1.0 + shift
        h12 = (rd - shift * rb) * (inv * inv_h21)
        k22 = (bd - shift * (bb + rd - shift * rb)) * (inv * inv_h21s)
        size = (dd - shift * (2.0 * bd - shift * bb)) * (inv * inv_h21s)
        h32s = size - h12 * h12 - k22 * k22
        h22 = 1.0 + k22
        m11 = h11 * h11 + h21s
        m12 = h11 * h12 + h21 * h22
        m22 = h12 * h12 + h22 * h22 + h32s
        inv_det = 1.0 / (m11 * m22 - m12 * m12)
        y1 = (m22 * h11 - m12 * h12) * inv_det
        y2 = (m11 * h12 - m12 * h11) * inv_det * inv_h21
        for q, x in enumerate((y1 - y2 * shift, y2, 1.0 - y1 + y2 * shift, y1 + y2 - y2 * shift)):
            for g in range(S // 8):
                coefs[q, 8 * g : 8 * (g + 1)] = jnp.broadcast_to(x[:, 8 * g : 8 * g + 1], (8, 128))

    with at("drain"):
        edges, zs_, ts_, gs = 4 * S * HALO * LEAF, 4 * (n_col - 1) * S * 128, 2 * (n_row - 1) * S * n_col * RANK, (total - 1) * 512
        arrived(wraw.at[pl.ds(0, (edges + zs_ + ts_ + gs) // 128)], sent)


def finish(rv, bv, dv, coefs, sol_hbm, res_hbm, sol, res, sem):
    width = rv.shape[1] // 2
    for g in range(S // 8):
        rows = slice(8 * g, 8 * (g + 1))
        sol_r, sol_b, res_r, res_b = (coefs[q, rows] for q in range(4))
        for part in range(2):
            for at in range(part * width, (part + 1) * width, 128):
                lanes = slice(at, at + 128)
                r, b, d = rv[rows, lanes], bv[rows, lanes], dv[rows, lanes]
                sol[rows, lanes] = sol_r * r + sol_b * b
                res[rows, lanes] = res_r * r - res_b * b - sol_b * d
            lanes = pl.ds(part * width, width)
            for k, (src, dst) in enumerate(((sol, sol_hbm), (res, res_hbm))):
                pltpu.make_async_copy(src.at[rows, lanes], dst.at[rows, lanes], sem.at[k]).start()
    for k, (src, dst) in enumerate(((sol, sol_hbm), (res, res_hbm))):
        pltpu.make_async_copy(src, dst, sem.at[k]).wait()


def solution(mesh):
    n_row, n_col = mesh.shape["row"], mesh.shape["col"]

    def body(rhs, near_blocks, near_offsets, v_factor, mix_col, mix_row, u_factor):
        leaves = near_offsets.shape[0]
        unknowns = leaves * LEAF
        w = near_blocks.reshape(leaves, 4, 32, 128).transpose(0, 2, 1, 3).reshape(leaves * 128, 128)
        by_tile = lambda x: x.reshape(leaves // 8, 8, 16, 128).transpose(0, 2, 1, 3).reshape(leaves * 16, 128)
        any_spec = pl.BlockSpec(memory_space=pl.ANY)
        field = pltpu.VMEM((S, unknowns), F32)
        vmem_spec = pl.BlockSpec(memory_space=pltpu.VMEM)
        parts = pl.pallas_call(
            functools.partial(kernel, n_row, n_col),
            out_shape=[field, field, field, pltpu.VMEM((4, S, 128), F32)],
            in_specs=[pl.BlockSpec(memory_space=pltpu.HBM)] * 7,
            out_specs=[vmem_spec] * 4,
            scratch_shapes=[
                pltpu.SMEM((4, leaves), jnp.int32),
                pltpu.VMEM((leaves * 128, 128), BF16),
                pltpu.VMEM((leaves * 64, 256), BF16),
                pltpu.VMEM((leaves * 16, 128), BF16),
                pltpu.VMEM((2, n_col, 256, 128), BF16),
                pltpu.VMEM((leaves * 16, 128), BF16),
                pltpu.VMEM((leaves * 32, 256), BF16),
                pltpu.VMEM(mix_col.shape[1:], BF16),
                pltpu.VMEM(mix_row.shape[1:], BF16),
                pltpu.VMEM((leaves + 2 * HALO, S, 128), BF16),
                pltpu.VMEM((256, 256), BF16),
                pltpu.VMEM((2, 2, S, HALO * LEAF), BF16),
                pltpu.VMEM((2, 2, S, HALO * LEAF), BF16),
                pltpu.VMEM((2, 2, n_col, S, 128), BF16),
                pltpu.VMEM((2, 2, n_col, S, 128), BF16),
                pltpu.VMEM((n_row, 4, S, 128), BF16),
                pltpu.VMEM((2, n_row, 4, S, 128), BF16),
                pltpu.VMEM((2, n_row, 4, S, 128), BF16),
                pltpu.VMEM((n_col, 2, S, 128), BF16),
                pltpu.VMEM((n_col, S, n_row * RANK), F32),
                pltpu.VMEM((2, n_col, S, 128), BF16),
                pltpu.VMEM((n_col, 128, 128), F32),
                pltpu.VMEM((16, 128, 128), F32),
                pltpu.VMEM((16, 128, 128), F32),
                pltpu.VMEM((2, 128), F32),
                pltpu.VMEM((n_row * n_col, 2, 128), F32),
                pltpu.SemaphoreType.DMA((7,)),
                pltpu.SemaphoreType.DMA,
                pltpu.SemaphoreType.DMA((2,)),
                pltpu.SemaphoreType.DMA((2, 2)),
                pltpu.SemaphoreType.DMA((2, 2)),
                pltpu.SemaphoreType.DMA,
            ],
            compiler_params=pltpu.CompilerParams(
                collective_id=0, has_side_effects=True, vmem_limit_bytes=54 * 1024 * 1024
            ),
        )(
            rhs, w, near_offsets.T, by_tile(v_factor),
            mix_col[0], mix_row[0], by_tile(u_factor),
        )
        return pl.pallas_call(
            finish,
            out_shape=[jax.ShapeDtypeStruct((S, unknowns), F32)] * 2,
            in_specs=[vmem_spec] * 4,
            out_specs=[any_spec] * 2,
            scratch_shapes=[
                pltpu.VMEM((S, unknowns), F32),
                pltpu.VMEM((S, unknowns), F32),
                pltpu.SemaphoreType.DMA((2,)),
            ],
            compiler_params=pltpu.CompilerParams(vmem_limit_bytes=8 * 1024 * 1024),
        )(*(pltpu.with_memory_space_constraint(x, pltpu.VMEM) for x in parts))

    both = ("row", "col")
    return jax.shard_map(
        body,
        mesh=mesh,
        in_specs=(
            P(None, both),
            P(both, None, None),
            P(both, None),
            P(both, None),
            P("row", "col", None, None),
            P("row", "col", None, None),
            P(both, None),
        ),
        out_specs=(P(None, both), P(None, both)),
        check_vma=False,
    )
```
